256 devices in a mesh: beam: 4 (over y, x), freq: 32 (over z), sub: 2 (over core).
Axes of the slice: x: 2, y: 2, z: 32, core: 2. Of those that a mesh axis runs over, the one named last changes fastest.
The devices are a block of a 4x8x32 slice.
Arguments:
- spectrum: bfloat16 [64, 4194304], P('sub', ('beam', 'freq')), parts along dimension 1
- hit_mask: int32 [64, 32768], P('sub', ('beam', 'freq')), parts along dimension 1, may hold values from 0 to 1, as said below
- owner_map: int32 [4096], P(('beam', 'freq')), parts along dimension 0, may hold values from 0 to 1023, as said below
- median_bin: int32 [4096], P(('beam', 'freq')), parts along dimension 0, may hold values from 32 to 559
- mad_bin: int32 [4096], P(('beam', 'freq')), parts along dimension 0, may hold values from 4 to 15
Outputs:
- hit_snr: bfloat16 [32, 2, 16384, 128], P('freq', 'sub', 'beam'), parts along dimension 2
- hit_keys: int32 [32, 2, 16384], P('freq', 'sub', 'beam'), parts along dimension 2
- hit_excess: float32 [32, 2, 16384], P('freq', 'sub', 'beam'), parts along dimension 2
The draws below stay inside these ranges and needn't reach their ends.
There are 4 independent parts, one for each index of `beam`. The reference program is written for one: setup_inputs(seed, part) draws one part's arguments, and reference() takes and returns one part's arrays. A program takes and returns all parts, laid end to end along the dimension named above; each array names one. Nothing has to cross between parts.
Inputs may be any that keep to these rules, and one draw needn't show every extreme that they name: `hit_mask`: for each index of freq, each half of the drift rates and each owner, at most 128 hit blocks go from the first to the last; in every draw some owner gets exactly 128 from every index of freq and half. `owner_map`: A permutation of the slots 0 to 1023; the 32 coarse channels of one index of freq go 1 to each owner, and the slot of index f's coarse channel at each owner is f.
All inputs are finite; a program needn't handle non-finite values.
Results may differ from the reference program's by a relative error of at most 0.007.
Values may be sent and summed in bfloat16 or wider, within the bound.
A program may use at most 64 MiB of HBM per device.

```python
import jax
import jax.numpy as jnp
from jax import lax

CHANNELS = 1048576
COARSE_WIDTH = 1024
BLOCK = 128
CAP = 128
DR_DEV = 32
DRIFTS = 64
COARSE = 1024
BPC = 8
NBLK = 8192
CD = 32
Q = 1
LIST = 4096
N_FREQ = 32
N_SUB = 2


def joint_draw(key):
    freq_count = COARSE // CD
    base = jax.random.fold_in(key, 101)
    parts = jax.random.split(base, 7)
    source_keys = jax.random.split(parts[0], freq_count)
    shuffled = jax.vmap(lambda one: jax.random.permutation(one, CD))(source_keys).astype(jnp.int32)
    source = jnp.arange(freq_count, dtype=jnp.int32)[:, None]
    owner = shuffled % freq_count
    local = source * Q + shuffled // freq_count
    owner_map = (owner * CD + local).reshape(COARSE).astype(jnp.int32)
    true_bin = jax.random.randint(parts[1], (COARSE,), 32, 160, dtype=jnp.int32)
    mad = jax.random.randint(parts[2], (COARSE,), 4, 16, dtype=jnp.int32)
    stale = (jax.random.randint(parts[3], (COARSE,), 0, 16, dtype=jnp.int32) == 0).astype(jnp.int32)
    median = true_bin + 400 * stale
    hot = jax.random.randint(parts[6], (), 0, freq_count, dtype=jnp.int32)
    dest = owner.reshape(COARSE)
    level = jax.random.randint(parts[4], (COARSE,), 0, 5, dtype=jnp.int32)
    limit = jnp.where(dest == hot, 1024, 32 * jnp.power(2, level)).astype(jnp.int32)
    tickets = jax.random.randint(parts[5], (DRIFTS, COARSE, BPC), 0, 1024, dtype=jnp.int32)
    raw = (tickets < limit[None, :, None]).astype(jnp.int32)
    half = (jnp.arange(DRIFTS, dtype=jnp.int32) // DR_DEV)[:, None, None]
    sender = (jnp.arange(COARSE, dtype=jnp.int32) // CD)[None, :, None]
    group = (half * freq_count + sender) * freq_count + dest[None, :, None]
    group = jnp.broadcast_to(group, (DRIFTS, COARSE, BPC)).reshape(-1)
    flat = raw.reshape(-1)
    groups_total = DRIFTS // DR_DEV * freq_count * freq_count
    order = jnp.argsort(group, stable=True)
    ordered = flat[order]
    running = jnp.cumsum(ordered).astype(jnp.int32)
    counts = jax.ops.segment_sum(flat, group, num_segments=groups_total)
    starts = (jnp.cumsum(counts) - counts).astype(jnp.int32)
    rank = running - starts[group[order]]
    keep = ordered * (rank <= CAP).astype(jnp.int32)
    mask = jnp.zeros_like(flat).at[order].set(keep).reshape(DRIFTS, COARSE, BPC)
    return (owner_map, median, mad, mask, true_bin)


def draw_owner_map(key, part):
    return joint_draw(key)[0]


def draw_median_bin(key, part):
    return joint_draw(key)[1]


def draw_mad_bin(key, part):
    return joint_draw(key)[2]


def draw_hit_mask(key, part):
    return joint_draw(key)[3].reshape(DRIFTS, NBLK)


def draw_spectrum(key, part):
    owner_map, median, mad, mask, true_bin = joint_draw(key)
    noise_key = jax.random.fold_in(key, 202)
    tone_key = jax.random.fold_in(key, 303)
    deviation = 1.4826 * 0.0625 * mad.astype(jnp.float32)
    center = 0.0625 * true_bin.astype(jnp.float32)
    ramp = 0.6 * jnp.power(3.0, jnp.arange(DRIFTS, dtype=jnp.float32) / max(DRIFTS - 1, 1))
    noise = jax.random.normal(noise_key, (DRIFTS, COARSE, BPC, BLOCK), jnp.float32)
    tone_at = jax.random.randint(tone_key, (DRIFTS, COARSE, BPC), 0, BLOCK, dtype=jnp.int32)
    tone = (jnp.arange(BLOCK, dtype=jnp.int32)[None, None, None, :] == tone_at[..., None]).astype(jnp.float32)
    tone = tone * mask[..., None].astype(jnp.float32)
    scale = deviation[None, :, None, None] * ramp[:, None, None, None]
    power = center[None, :, None, None] + scale * noise + 8.0 * scale * tone
    return power.reshape(DRIFTS, CHANNELS).astype(jnp.bfloat16)


def setup_inputs(seed: int = 0, part: int = 0) -> dict:
    key_of = jax.random.split(jax.random.key(seed), 6)
    own_keys = jax.random.split(jax.random.fold_in(key_of[5], part), 6)
    return {
        "spectrum": draw_spectrum(jax.random.fold_in(jax.random.fold_in(key_of[5], part), 71), part),
        "hit_mask": draw_hit_mask(jax.random.fold_in(jax.random.fold_in(key_of[5], part), 71), part),
        "owner_map": draw_owner_map(jax.random.fold_in(jax.random.fold_in(key_of[5], part), 71), part),
        "median_bin": draw_median_bin(jax.random.fold_in(jax.random.fold_in(key_of[5], part), 71), part),
        "mad_bin": draw_mad_bin(jax.random.fold_in(jax.random.fold_in(key_of[5], part), 71), part),
    }


BIN_STEP = 0.0625
MAD_WIDTH = 5.0
MAD_SCALE = 1.4826
THRESH = 3.0

def reference(spectrum, hit_mask, owner_map, median_bin, mad_bin):
    per_coarse = COARSE_WIDTH // BLOCK
    power = spectrum.astype(jnp.float32).reshape(DRIFTS, COARSE, COARSE_WIDTH)
    center = BIN_STEP * median_bin.astype(jnp.float32)
    spread = MAD_WIDTH * BIN_STEP * mad_bin.astype(jnp.float32)
    inside = (power >= (center - spread)[None, :, None]) & (power <= (center + spread)[None, :, None])
    kept = jnp.where(inside, power - center[None, :, None], jnp.float32(0.0))
    count = lax.optimization_barrier(jnp.sum(inside.astype(jnp.float32), axis=(0, 2)))
    first = lax.optimization_barrier(jnp.sum(kept, axis=(0, 2)))
    second = lax.optimization_barrier(jnp.sum(kept * kept, axis=(0, 2)))
    floor_count = jnp.maximum(count, 1.0)
    mean_level = center + first / floor_count
    mad_sigma = MAD_SCALE * BIN_STEP * mad_bin.astype(jnp.float32)
    sigma = jnp.sqrt(0.5 * second / floor_count + 0.5 * mad_sigma * mad_sigma)
    snr = ((power - mean_level[None, :, None]) / sigma[None, :, None]).astype(jnp.bfloat16)
    snr = snr.reshape(DRIFTS, COARSE, per_coarse, BLOCK)
    inverse = jnp.zeros((COARSE,), jnp.int32).at[owner_map].set(jnp.arange(COARSE, dtype=jnp.int32))
    by_slot = snr[:, inverse]
    marks = hit_mask.reshape(DRIFTS, COARSE, per_coarse)[:, inverse]
    by_slot = by_slot.reshape(N_SUB, DR_DEV, N_FREQ, CD, per_coarse, BLOCK).transpose(2, 0, 3, 1, 4, 5)
    by_slot = by_slot.reshape(N_FREQ * N_SUB, CD * DR_DEV * per_coarse, BLOCK)
    marks = marks.reshape(N_SUB, DR_DEV, N_FREQ, CD, per_coarse).transpose(2, 0, 3, 1, 4)
    marks = marks.reshape(N_FREQ * N_SUB, CD * DR_DEV * per_coarse).astype(jnp.int32)
    slots = jnp.arange(CD, dtype=jnp.int32)[None, None, :, None, None]
    halves = jnp.arange(N_SUB, dtype=jnp.int32)[None, :, None, None, None]
    drifts = jnp.arange(DR_DEV, dtype=jnp.int32)[None, None, None, :, None]
    blocks = jnp.arange(per_coarse, dtype=jnp.int32)[None, None, None, None, :]
    keys = (slots * DRIFTS + halves * DR_DEV + drifts) * per_coarse + blocks
    keys = jnp.broadcast_to(keys, (N_FREQ, N_SUB, CD, DR_DEV, per_coarse)).reshape(N_FREQ * N_SUB, -1)
    place = jnp.where(marks > 0, jnp.cumsum(marks, axis=-1).astype(jnp.int32) - 1, LIST).astype(jnp.int32)

    def collect(items):
        rows, key_row, place_row = items
        snr_list = jnp.zeros((LIST, BLOCK), jnp.bfloat16).at[place_row].set(rows, mode='drop')
        key_list = jnp.full((LIST,), -1, jnp.int32).at[place_row].set(key_row, mode='drop')
        excess = lax.optimization_barrier(jnp.sum(jnp.maximum(snr_list.astype(jnp.float32) - THRESH, 0.0), axis=-1))
        return (snr_list, key_list, excess)
    snr_lists, key_lists, excess = lax.map(collect, (by_slot, keys, place))
    return (snr_lists.reshape(N_FREQ, N_SUB, LIST, BLOCK), key_lists.reshape(N_FREQ, N_SUB, LIST), excess.reshape(N_FREQ, N_SUB, LIST))
```

```python
import functools

import jax
import jax.numpy as jnp
from jax import lax
from jax.experimental import pallas as pl
from jax.experimental.pallas import tpu as pltpu
from jax.sharding import PartitionSpec as P

COARSE_WIDTH = 1024
BLOCK = 128
CAP = 128
PER = COARSE_WIDTH // BLOCK

BIN_STEP = 0.0625
MAD_WIDTH = 5.0
MAD_SCALE = 1.4826
THRESH = 3.0

VMEM = pltpu.VMEM
SMEM = pltpu.SMEM
MESH = pl.DeviceIdType.MESH
F32 = jnp.float32
BF16 = jnp.bfloat16


def dot_nt(a, b):
    return lax.dot_general(a, b, (((1,), (1,)), ((), ())), preferred_element_type=F32)


def stats_kernel(coarse, low, high, mid, spec, center, mad, mean_out, sigma_out, mine, theirs, sems):
    other = 1 - lax.axis_index("sub")
    barrier = pltpu.get_barrier_semaphore()
    pl.semaphore_signal(barrier, inc=1, device_id={"sub": other}, device_id_type=MESH)

    def one(c, carry):
        lo, hi, at = low[c], high[c], mid[c]
        count = first = second = None
        for b in range(PER):
            x = spec[:, pl.ds(pl.multiple_of(c * COARSE_WIDTH + b * BLOCK, BLOCK), BLOCK)].astype(F32)
            inside = (x >= lo) & (x <= hi)
            kept = jnp.where(inside, x - at, 0.0)
            ones = jnp.where(inside, 1.0, 0.0)
            square = kept * kept
            count = ones if b == 0 else count + ones
            first = kept if b == 0 else first + kept
            second = square if b == 0 else second + square
        mine[0, pl.ds(c, 1), :] = jnp.sum(count, axis=0, keepdims=True)
        mine[1, pl.ds(c, 1), :] = jnp.sum(first, axis=0, keepdims=True)
        mine[2, pl.ds(c, 1), :] = jnp.sum(second, axis=0, keepdims=True)
        return carry

    lax.fori_loop(0, coarse, one, 0, unroll=2)
    pl.semaphore_wait(barrier, 1)
    copy = pltpu.make_async_remote_copy(
        src_ref=mine, dst_ref=theirs, send_sem=sems.at[0], recv_sem=sems.at[1],
        device_id={"sub": other}, device_id_type=MESH,
    )
    copy.start()
    copy.wait()
    total = [jnp.sum(mine[k] + theirs[k], axis=1, keepdims=True) for k in range(3)]
    floor = jnp.maximum(total[0], 1.0)
    mean = center[...] + total[1] / floor
    mad_sigma = MAD_SCALE * BIN_STEP * mad[...]
    sigma = jnp.sqrt(0.5 * total[2] / floor + 0.5 * mad_sigma * mad_sigma)
    mean_out[...] = jnp.broadcast_to(mean, mean_out.shape)
    sigma_out[...] = jnp.broadcast_to(sigma, sigma_out.shape)


def displacement(i, n):
    step = n // 2 - i // 2
    return jnp.where(i == 0, 0, jnp.where(i % 2 == 1, step, n - step))


def exchange_kernel(
    n, drift, total_drift, source_of, spec, marks, mean, sigma,
    rows, keys, excess, begins,
    rank, filled, send_rows, send_codes, got_codes, row_sems, code_sems,
):
    me = lax.axis_index("freq")
    half = lax.axis_index("sub")
    barrier = pltpu.get_barrier_semaphore()

    def greet(i, carry):
        pl.semaphore_signal(barrier, inc=1, device_id={"freq": (me + i) % n}, device_id_type=MESH)
        return carry

    lax.fori_loop(1, n, greet, 0)
    width = PER * drift

    def position(at):
        tile, block, row = at // (PER * 8), at // 8 % PER, at % 8
        return (tile * 8 + row) * PER + block

    def order(axis):
        return position(lax.broadcasted_iota(jnp.int32, (width, width), axis))

    before = jnp.where(order(0) < order(1), 1.0, 0.0).astype(BF16)
    set_here = marks[...]
    mark_float = set_here.astype(F32)
    ranks = jnp.dot(mark_float.astype(BF16), before, preferred_element_type=F32)
    rank[...] = jnp.where(set_here > 0, ranks, -1.0)
    filled[...] = jnp.broadcast_to(jnp.sum(mark_float, axis=1, keepdims=True), filled.shape)
    at = lax.broadcasted_iota(jnp.int32, (8, width), 1)
    code = (position(at) + 1).astype(F32).astype(BF16)
    slot_wide = lax.broadcasted_iota(jnp.int32, (CAP, width), 0).astype(F32)
    slot = lax.broadcasted_iota(jnp.int32, (CAP, BLOCK), 0).astype(F32)

    def build(owner):
        c = source_of[owner]
        chosen = jnp.where(slot_wide == rank[pl.ds(c, 1), :], 1.0, 0.0).astype(BF16)
        blocks = spec[:, pl.ds(c * PER, PER)].reshape(width, BLOCK)
        power = jnp.dot(chosen, blocks, preferred_element_type=F32)
        normal = (power - mean[pl.ds(c, 1), :]) / sigma[pl.ds(c, 1), :]
        payload = jnp.where(slot < filled[pl.ds(c, 1), :], normal, 0.0).astype(BF16)
        return payload, dot_nt(code, chosen)[0:1]

    payload, codes = build(me)
    rows[me] = payload
    got_codes[me] = codes

    def pack(i, carry):
        payload, codes = build((me + displacement(i, n)) % n)
        send_rows[i] = payload
        send_codes[i] = codes
        return carry

    lax.fori_loop(1, n, pack, 0, unroll=2)

    def code_copy(i):
        return pltpu.make_async_remote_copy(
            src_ref=send_codes.at[i], dst_ref=got_codes.at[me],
            send_sem=code_sems.at[0, i], recv_sem=code_sems.at[1, i],
            device_id={"freq": (me + displacement(i, n)) % n}, device_id_type=MESH,
        )

    def row_copy(i):
        return pltpu.make_async_remote_copy(
            src_ref=send_rows.at[i], dst_ref=rows.at[me],
            send_sem=row_sems.at[0, i], recv_sem=row_sems.at[1, i],
            device_id={"freq": (me + displacement(i, n)) % n}, device_id_type=MESH,
        )

    pl.semaphore_wait(barrier, n - 1)

    def start_codes(i, carry):
        code_copy(i).start()
        return carry

    def start_rows(i, carry):
        row_copy(i).start()
        return carry

    lax.fori_loop(1, n, start_codes, 0)
    lax.fori_loop(1, n, start_rows, 0)
    ones = jnp.ones((8, BLOCK), BF16)

    def take_codes(sender):
        codes = got_codes[sender]
        base = (sender * total_drift + half * drift) * PER - 1
        keys[pl.ds(sender, 1), :] = jnp.where(codes > 0, codes + base.astype(F32), -1.0)

    def take_rows(sender):
        over = jnp.maximum(rows[sender].astype(F32) - THRESH, 0.0)
        coarse_part = over.astype(BF16)
        fine_part = (over - coarse_part.astype(F32)).astype(BF16)
        excess[pl.ds(sender, 1), :] = (dot_nt(ones, coarse_part) + dot_nt(ones, fine_part))[0:1]

    take_codes(me)
    take_rows(me)

    def codes_in(i, carry):
        code_copy(i).wait()
        take_codes((me + n - displacement(i, n)) % n)
        return carry

    def rows_in(i, carry):
        row_copy(i).wait()
        take_rows((me + n - displacement(i, n)) % n)
        return carry

    lax.fori_loop(1, n, codes_in, 0)
    live = jnp.where(keys[...] >= 0, 1.0, 0.0).astype(BF16)
    counts = dot_nt(ones, live)
    earlier = jnp.where(
        lax.broadcasted_iota(jnp.int32, (n, n), 0) < lax.broadcasted_iota(jnp.int32, (n, n), 1), 1.0, 0.0
    ).astype(BF16)
    begins[...] = jnp.dot(counts.astype(BF16), earlier, preferred_element_type=F32).astype(jnp.int32)
    lax.fori_loop(1, n, rows_in, 0)


def compact_kernel(n, begins, rows, keys, excess, snr_out, keys_out, excess_out, wide, key_rows, excess_rows):
    wide[...] = jnp.zeros_like(wide)
    key_rows[...] = jnp.full_like(key_rows, -1.0)
    excess_rows[...] = jnp.zeros_like(excess_rows)
    lane = lax.broadcasted_iota(jnp.int32, (1, BLOCK), 1)
    for s in range(n):
        begin = begins[0, s]
        wide[pl.ds(begin, CAP), :] = rows[s].astype(F32)
        row, shift = begin // BLOCK, begin % BLOCK
        for source, target, empty in ((keys, key_rows, -1.0), (excess, excess_rows, 0.0)):
            turned = pltpu.roll(source[pl.ds(s, 1), :], shift, 1)
            here, after = pl.ds(row, 1), pl.ds(row + 1, 1)
            target[here, :] = jnp.where(lane >= shift, turned, target[here, :])
            target[after, :] = jnp.where(lane < shift, turned, empty)
    snr_out[...] = wide[...].astype(BF16)
    keys_out[...] = key_rows[0:n, :].astype(jnp.int32)
    excess_out[...] = excess_rows[0:n, :]


def per_device(spectrum, hit_mask, owner_map, median_bin, mad_bin):
    drift = spectrum.shape[0]
    coarse = owner_map.shape[0]
    n = lax.axis_size("freq")
    total_drift = drift * lax.axis_size("sub")
    width = PER * drift
    center = BIN_STEP * median_bin.astype(F32)
    mad = mad_bin.astype(F32)
    spread = MAD_WIDTH * BIN_STEP * mad
    vmem, smem = pl.BlockSpec(memory_space=VMEM), pl.BlockSpec(memory_space=SMEM)
    mean, sigma = pl.pallas_call(
        functools.partial(stats_kernel, coarse),
        out_shape=[jax.ShapeDtypeStruct((coarse, BLOCK), F32)] * 2,
        in_specs=[smem] * 3 + [vmem] * 3,
        out_specs=[vmem] * 2,
        scratch_shapes=[
            VMEM((3, coarse, BLOCK), F32), VMEM((3, coarse, BLOCK), F32), pltpu.SemaphoreType.DMA((2,)),
        ],
        compiler_params=pltpu.CompilerParams(collective_id=1, has_side_effects=True),
        name="stats",
    )(center - spread, center + spread, center, spectrum, center[:, None], mad[:, None])
    tiles = spectrum.reshape(drift // 8, 8, coarse * PER, BLOCK).transpose(0, 2, 1, 3)
    marks = hit_mask.reshape(drift // 8, 8, coarse, PER).transpose(2, 0, 3, 1).reshape(coarse, width)
    dest = owner_map // coarse
    owners = jnp.arange(n, dtype=jnp.int32)
    source_of = jnp.sum(
        jnp.where(dest[None, :] == owners[:, None], jnp.arange(coarse, dtype=jnp.int32)[None, :], 0), axis=1
    )
    rows, keys, excess, begins = pl.pallas_call(
        functools.partial(exchange_kernel, n, drift, total_drift),
        out_shape=[
            jax.ShapeDtypeStruct((n, CAP, BLOCK), BF16),
            jax.ShapeDtypeStruct((n, BLOCK), F32),
            jax.ShapeDtypeStruct((n, BLOCK), F32),
            jax.ShapeDtypeStruct((8, n), jnp.int32),
        ],
        in_specs=[smem] + [vmem] * 4,
        out_specs=[vmem] * 4,
        scratch_shapes=[
            VMEM((coarse, width), F32), VMEM((coarse, BLOCK), F32),
            VMEM((n, CAP, BLOCK), BF16), VMEM((n, 1, CAP), F32), VMEM((n, 1, CAP), F32),
            pltpu.SemaphoreType.DMA((2, n)), pltpu.SemaphoreType.DMA((2, n)),
        ],
        compiler_params=pltpu.CompilerParams(collective_id=0, has_side_effects=True),
        name="exchange",
    )(source_of, tiles, marks, mean, sigma)
    snr, keys, excess = pl.pallas_call(
        functools.partial(compact_kernel, n),
        out_shape=[
            jax.ShapeDtypeStruct((n * CAP, BLOCK), BF16),
            jax.ShapeDtypeStruct((n, BLOCK), jnp.int32),
            jax.ShapeDtypeStruct((n, BLOCK), F32),
        ],
        in_specs=[smem] + [vmem] * 3,
        out_specs=[vmem] * 3,
        scratch_shapes=[VMEM((n * CAP, BLOCK), F32), VMEM((n + 8, BLOCK), F32), VMEM((n + 8, BLOCK), F32)],
        name="compact",
    )(begins, rows, keys, excess)
    total = n * CAP
    return snr.reshape(1, 1, total, BLOCK), keys.reshape(1, 1, total), excess.reshape(1, 1, total)


def solution(mesh):
    placed = (
        P("sub", ("beam", "freq")),
        P("sub", ("beam", "freq")),
        P(("beam", "freq")),
        P(("beam", "freq")),
        P(("beam", "freq")),
    )
    return jax.shard_map(
        per_device,
        mesh=mesh,
        in_specs=placed,
        out_specs=(
            P("freq", "sub", "beam", None),
            P("freq", "sub", "beam"),
            P("freq", "sub", "beam"),
        ),
        check_vma=False,
    )
```

```python
import functools

import jax
import jax.numpy as jnp
from jax import lax
from jax.experimental import pallas as pl
from jax.experimental.pallas import tpu as pltpu
from jax.sharding import PartitionSpec as P

COARSE_WIDTH = 1024
BLOCK = 128
CAP = 128
PER = COARSE_WIDTH // BLOCK

BIN_STEP = 0.0625
MAD_WIDTH = 5.0
MAD_SCALE = 1.4826
THRESH = 3.0

VMEM = pltpu.VMEM
SMEM = pltpu.SMEM
MESH = pl.DeviceIdType.MESH
F32 = jnp.float32
BF16 = jnp.bfloat16


def dot_nt(a, b):
    return lax.dot_general(a, b, (((1,), (1,)), ((), ())), preferred_element_type=F32)


REACH = 4


def exchange_kernel(
    n, coarse, drift, total_drift,
    owner_hbm, median_hbm, mad_hbm, marks_hbm, spec_hbm,
    rows, keys, excess, begins,
    owner, median, mad, source_of, marks, spec, mine, theirs, mean, sigma, rank, filled,
    send_rows, send_codes, got_codes,
    small_sems, spec_sems, stat_sems, row_sems, code_sems, chain,
):
    me = lax.axis_index("freq")
    half = lax.axis_index("sub")
    far = n // 2
    rounds = far // REACH - 1
    groups = spec_sems.shape[0]
    group = coarse // groups
    width = PER * drift
    barrier = pltpu.get_barrier_semaphore()
    small = [
        pltpu.make_async_copy(src, dst, small_sems.at[k])
        for k, (src, dst) in enumerate(
            ((owner_hbm, owner), (median_hbm, median), (mad_hbm, mad), (marks_hbm, marks))
        )
    ]
    large = []
    for g in range(groups):
        part = pl.ds(g * group * PER, group * PER)
        large.append(pltpu.make_async_copy(spec_hbm.at[:, part], spec.at[:, part], spec_sems.at[g]))
    for copy in small + large:
        copy.start()
    pl.semaphore_signal(barrier, inc=1, device_id={"sub": 1 - half}, device_id_type=MESH)
    for d in range(1, REACH + 1):
        for to in (me + d, me + n - d):
            pl.semaphore_signal(barrier, inc=1, device_id={"freq": to % n}, device_id_type=MESH)

    for copy in small:
        copy.wait()

    def position(at):
        tile, block, row = at // (PER * 8), at // 8 % PER, at % 8
        return (tile * 8 + row) * PER + block

    def iota(shape, axis):
        return lax.broadcasted_iota(jnp.int32, shape, axis)

    def hot(mask):
        return jnp.where(mask, 1.0, 0.0).astype(BF16)

    lanes = coarse * PER
    spread = hot(iota((lanes, lanes), 1) == iota((lanes, lanes), 0) % coarse * PER + iota((lanes, lanes), 0) // coarse)
    by_block = dot_nt(spread, marks[...].astype(F32).astype(BF16)).astype(BF16)
    ranks = set_here = None
    for b in range(PER):
        here = by_block[b * coarse : (b + 1) * coarse]
        come, go = iota((drift, width), 0) * PER + b, position(iota((drift, width), 1))
        before = jnp.dot(here, hot(come < go), preferred_element_type=F32)
        same = jnp.dot(here, hot(come == go), preferred_element_type=F32)
        ranks = before if b == 0 else ranks + before
        set_here = same if b == 0 else set_here + same
    rank[...] = jnp.where(set_here > 0, ranks, -1.0)
    filled[...] = jnp.broadcast_to(jnp.sum(set_here, axis=1, keepdims=True), filled.shape)

    def stats(c, carry):
        center = BIN_STEP * median[c].astype(F32)
        deviation = mad[c].astype(F32)
        wide = MAD_WIDTH * BIN_STEP * deviation
        mean[pl.ds(c, 1), :] = jnp.full((1, BLOCK), center, F32)
        sigma[pl.ds(c, 1), :] = jnp.full((1, BLOCK), MAD_SCALE * BIN_STEP * deviation, F32)
        found = 0
        for k in range(coarse):
            found = jnp.where(owner[k] == c * coarse + me, k, found)
        source_of[c] = found
        x = spec[:, pl.ds(c * PER, PER)].astype(F32)
        inside = (x >= center - wide) & (x <= center + wide)
        kept = jnp.where(inside, x - center, 0.0)
        for k, each in enumerate((jnp.where(inside, 1.0, 0.0), kept, kept * kept)):
            mine[k, pl.ds(c, 1), :] = jnp.sum(jnp.sum(each, axis=(0, 1)), axis=0, keepdims=True)
        return carry

    for g in range(groups):
        large[g].wait()
        lax.fori_loop(g * group, (g + 1) * group, stats, 0)

    pl.semaphore_wait(barrier, 2 * REACH + 1)

    def tell(k):
        for to in (me + REACH, me + n - REACH):
            pl.semaphore_signal(chain.at[k], inc=1, device_id={"freq": to % n}, device_id_type=MESH)

    share = pltpu.make_async_remote_copy(
        src_ref=mine, dst_ref=theirs, send_sem=stat_sems.at[0], recv_sem=stat_sems.at[1],
        device_id={"sub": 1 - half}, device_id_type=MESH,
    )
    share.start()
    if rounds:
        tell(0)

    def hear(k):
        if k < rounds:
            pl.semaphore_wait(chain.at[k], 2)
            if k + 1 < rounds:
                tell(k + 1)

    at = iota((8, width), 1)
    code = (position(at) + 1).astype(F32).astype(BF16)
    slot_wide = iota((CAP, width), 0).astype(F32)
    slot = iota((CAP, BLOCK), 0).astype(F32)
    share.wait()
    total = [jnp.sum(mine[k] + theirs[k], axis=1, keepdims=True) for k in range(3)]
    floor = jnp.maximum(total[0], 1.0)
    mean[...] = mean[...] + total[1] / floor
    sigma[...] = jnp.sqrt(0.5 * total[2] / floor + 0.5 * sigma[...] * sigma[...])

    def build(to):
        c = source_of[to]
        chosen = hot(slot_wide == rank[pl.ds(c, 1), :])
        blocks = spec[:, pl.ds(c * PER, PER)].reshape(width, BLOCK)
        power = jnp.dot(chosen, blocks, preferred_element_type=F32)
        normal = (power - mean[pl.ds(c, 1), :]) / sigma[pl.ds(c, 1), :]
        payload = jnp.where(slot < filled[pl.ds(c, 1), :], normal, 0.0).astype(BF16)
        return payload, dot_nt(code, chosen)[0:1]

    def pack(d):
        payload, codes = build((me + d) % n)
        send_rows[d] = payload
        send_codes[d] = codes

    def code_copy(d):
        return pltpu.make_async_remote_copy(
            src_ref=send_codes.at[d], dst_ref=got_codes.at[me],
            send_sem=code_sems.at[0, d], recv_sem=code_sems.at[1, d],
            device_id={"freq": (me + d) % n}, device_id_type=MESH,
        )

    def row_copy(d):
        return pltpu.make_async_remote_copy(
            src_ref=send_rows.at[d], dst_ref=rows.at[me],
            send_sem=row_sems.at[0, d], recv_sem=row_sems.at[1, d],
            device_id={"freq": (me + d) % n}, device_id_type=MESH,
        )

    def send(d):
        code_copy(d).start()
        row_copy(d).start()

    def each(first, last, act):
        def body(k, carry):
            m = first - k
            act(m)
            act(n - m)
            return carry
        lax.fori_loop(0, first - last + 1, body, 0)

    def pack_send(ms):
        waiting = []
        for d in [d for m in ms for d in (m, n - m)]:
            pack(d)
            if waiting:
                send(waiting.pop())
            waiting.append(d)
        send(waiting.pop())

    early = [m for m in (2, 4, 3) if m <= REACH and m < far]
    middle = [m for m in (6,) if REACH < m <= 2 * REACH and m < far]
    near = [m for m in range(2 * REACH, 0, -1) if m not in early + middle and m < far]
    top = far - 1
    deep = max(top - 3, 2 * REACH + 1)
    pack_send(early)
    hear(0)
    if middle:
        pack_send(middle)
    if far > 2 * REACH:
        pack(far)
        each(top, deep, pack)
        hear(1)
        if deep > 2 * REACH + 1:
            each(deep - 1, 2 * REACH + 1, pack)
        for k in range(2, rounds):
            hear(k)
        send(far)
        each(top, 2 * REACH + 1, send)
    else:
        pack(far)
        send(far)
    if near:
        pack_send(near)

    ones = jnp.ones((8, BLOCK), BF16)

    def take(sender):
        codes = got_codes[sender]
        base = (sender * total_drift + half * drift) * PER - 1
        keys[pl.ds(sender, 1), :] = jnp.where(codes > 0, codes + base.astype(F32), -1.0)
        over = jnp.maximum(rows[sender].astype(F32) - THRESH, 0.0)
        coarse_part = over.astype(BF16)
        fine_part = (over - coarse_part.astype(F32)).astype(BF16)
        excess[pl.ds(sender, 1), :] = (dot_nt(ones, coarse_part) + dot_nt(ones, fine_part))[0:1]

    def arrive(d):
        code_copy(d).wait()
        row_copy(d).wait()
        take((me + n - d) % n)

    payload, codes = build(me)
    rows[me] = payload
    got_codes[me] = codes
    take(me)
    for m in early + middle:
        arrive(m)
        arrive(n - m)
    arrive(far)
    if far > 2 * REACH:
        each(top, 2 * REACH + 1, arrive)
    for m in near:
        arrive(m)
        arrive(n - m)
    counts = dot_nt(ones, hot(keys[...] >= 0))
    earlier = hot(iota((n, n), 0) < iota((n, n), 1))
    begins[...] = jnp.dot(counts.astype(BF16), earlier, preferred_element_type=F32).astype(jnp.int32)


def compact_kernel(n, begins, rows, keys, excess, snr_out, keys_out, excess_out, wide, key_rows, excess_rows):
    wide[...] = jnp.zeros_like(wide)
    key_rows[...] = jnp.full_like(key_rows, -1.0)
    excess_rows[...] = jnp.zeros_like(excess_rows)
    lane = lax.broadcasted_iota(jnp.int32, (1, BLOCK), 1)
    for s in range(n):
        begin = begins[0, s]
        wide[pl.ds(begin, CAP), :] = rows[s].astype(F32)
        row, shift = begin // BLOCK, begin % BLOCK
        for source, target, empty in ((keys, key_rows, -1.0), (excess, excess_rows, 0.0)):
            turned = pltpu.roll(source[pl.ds(s, 1), :], shift, 1)
            here, after = pl.ds(row, 1), pl.ds(row + 1, 1)
            target[here, :] = jnp.where(lane >= shift, turned, target[here, :])
            target[after, :] = jnp.where(lane < shift, turned, empty)
    snr_out[...] = wide[...].astype(BF16)
    keys_out[...] = key_rows[0:n, :].astype(jnp.int32)
    excess_out[...] = excess_rows[0:n, :]


def per_device(spectrum, hit_mask, owner_map, median_bin, mad_bin):
    drift = spectrum.shape[0]
    coarse = owner_map.shape[0]
    n = lax.axis_size("freq")
    total_drift = drift * lax.axis_size("sub")
    width = PER * drift
    vmem, smem = pl.BlockSpec(memory_space=VMEM), pl.BlockSpec(memory_space=SMEM)
    tiles = spectrum.reshape(drift // 8, 8, coarse * PER, BLOCK).transpose(0, 2, 1, 3)
    table = VMEM((coarse, BLOCK), F32)
    dma = pltpu.SemaphoreType.DMA
    rows, keys, excess, begins = pl.pallas_call(
        functools.partial(exchange_kernel, n, coarse, drift, total_drift),
        out_shape=[
            jax.ShapeDtypeStruct((n, CAP, BLOCK), BF16),
            jax.ShapeDtypeStruct((n, BLOCK), F32),
            jax.ShapeDtypeStruct((n, BLOCK), F32),
            jax.ShapeDtypeStruct((8, n), jnp.int32),
        ],
        in_specs=[pl.BlockSpec(memory_space=pl.ANY)] * 5,
        out_specs=[vmem] * 4,
        scratch_shapes=[
            SMEM((coarse,), jnp.int32), SMEM((coarse,), jnp.int32), SMEM((coarse,), jnp.int32),
            SMEM((coarse,), jnp.int32),
            VMEM(hit_mask.shape, jnp.int32), VMEM(tiles.shape, BF16),
            VMEM((3, coarse, BLOCK), F32), VMEM((3, coarse, BLOCK), F32), table, table,
            VMEM((coarse, width), F32), table,
            VMEM((n, CAP, BLOCK), BF16), VMEM((n, 1, CAP), F32), VMEM((n, 1, CAP), F32),
            dma((4,)), dma((4,)), dma((2,)), dma((2, n)), dma((2, n)),
            pltpu.SemaphoreType.REGULAR((max(n // 2 // REACH - 1, 1),)),
        ],
        compiler_params=pltpu.CompilerParams(collective_id=0, has_side_effects=True),
        name="exchange",
    )(owner_map, median_bin, mad_bin, hit_mask, tiles)
    snr, keys, excess = pl.pallas_call(
        functools.partial(compact_kernel, n),
        out_shape=[
            jax.ShapeDtypeStruct((n * CAP, BLOCK), BF16),
            jax.ShapeDtypeStruct((n, BLOCK), jnp.int32),
            jax.ShapeDtypeStruct((n, BLOCK), F32),
        ],
        in_specs=[smem] + [vmem] * 3,
        out_specs=[vmem] * 3,
        scratch_shapes=[VMEM((n * CAP, BLOCK), F32), VMEM((n + 8, BLOCK), F32), VMEM((n + 8, BLOCK), F32)],
        name="compact",
    )(begins, rows, keys, excess)
    total = n * CAP
    return snr.reshape(1, 1, total, BLOCK), keys.reshape(1, 1, total), excess.reshape(1, 1, total)


def solution(mesh):
    placed = (
        P("sub", ("beam", "freq")),
        P("sub", ("beam", "freq")),
        P(("beam", "freq")),
        P(("beam", "freq")),
        P(("beam", "freq")),
    )
    return jax.shard_map(
        per_device,
        mesh=mesh,
        in_specs=placed,
        out_specs=(
            P("freq", "sub", "beam", None),
            P("freq", "sub", "beam"),
            P("freq", "sub", "beam"),
        ),
        check_vma=False,
    )
```

```python
import functools

import jax
import jax.numpy as jnp
from jax import lax
from jax.experimental import pallas as pl
from jax.experimental.pallas import tpu as pltpu
from jax.sharding import PartitionSpec as P

COARSE_WIDTH = 1024
BLOCK = 128
CAP = 128
PER = COARSE_WIDTH // BLOCK

BIN_STEP = 0.0625
MAD_WIDTH = 5.0
MAD_SCALE = 1.4826
THRESH = 3.0

VMEM = pltpu.VMEM
SMEM = pltpu.SMEM
MESH = pl.DeviceIdType.MESH
F32 = jnp.float32
BF16 = jnp.bfloat16


def dot_nt(a, b):
    return lax.dot_general(a, b, (((1,), (1,)), ((), ())), preferred_element_type=F32)


REACH = 4


def exchange_kernel(
    n, coarse, drift, total_drift,
    owner_hbm, median_hbm, mad_hbm, marks_hbm, spec_hbm,
    rows, keys, excess, begins,
    owner, median, mad, source_of, marks, spec, mine, theirs, mean, sigma, rank, filled,
    send_rows, send_codes, got_codes, send_norms, got_norms,
    small_sems, spec_sems, stat_sems, row_sems, code_sems, norm_sems, chain,
):
    me = lax.axis_index("freq")
    half = lax.axis_index("sub")
    far = n // 2
    rounds = far // REACH - 1
    groups = spec_sems.shape[0]
    group = coarse // groups
    width = PER * drift
    barrier = pltpu.get_barrier_semaphore()
    small = [
        pltpu.make_async_copy(src, dst, small_sems.at[k])
        for k, (src, dst) in enumerate(
            ((owner_hbm, owner), (median_hbm, median), (mad_hbm, mad), (marks_hbm, marks))
        )
    ]
    large = []
    for g in range(groups):
        part = pl.ds(g * group * PER, group * PER)
        large.append(pltpu.make_async_copy(spec_hbm.at[:, part], spec.at[:, part], spec_sems.at[g]))
    for copy in small + large:
        copy.start()
    pl.semaphore_signal(barrier, inc=1, device_id={"sub": 1 - half}, device_id_type=MESH)
    for d in range(1, REACH + 1):
        for to in (me + d, me + n - d):
            pl.semaphore_signal(barrier, inc=1, device_id={"freq": to % n}, device_id_type=MESH)

    for copy in small:
        copy.wait()

    def position(at):
        tile, block, row = at // (PER * 8), at // 8 % PER, at % 8
        return (tile * 8 + row) * PER + block

    def iota(shape, axis):
        return lax.broadcasted_iota(jnp.int32, shape, axis)

    def hot(mask):
        return jnp.where(mask, 1.0, 0.0).astype(BF16)

    lanes = coarse * PER
    spread = hot(iota((lanes, lanes), 1) == iota((lanes, lanes), 0) % coarse * PER + iota((lanes, lanes), 0) // coarse)
    by_block = dot_nt(spread, marks[...].astype(F32).astype(BF16)).astype(BF16)
    ranks = set_here = None
    for b in range(PER):
        here = by_block[b * coarse : (b + 1) * coarse]
        come, go = iota((drift, width), 0) * PER + b, position(iota((drift, width), 1))
        before = jnp.dot(here, hot(come < go), preferred_element_type=F32)
        same = jnp.dot(here, hot(come == go), preferred_element_type=F32)
        ranks = before if b == 0 else ranks + before
        set_here = same if b == 0 else set_here + same
    rank[...] = jnp.where(set_here > 0, ranks, -1.0)
    filled[...] = jnp.broadcast_to(jnp.sum(set_here, axis=1, keepdims=True), filled.shape)

    early = [m for m in (2, 4, 3) if m <= REACH and m < far]
    middle = [m for m in (6,) if REACH < m <= 2 * REACH and m < far]
    late = [m for m in range(far - 1, 0, -1) if m not in early + middle]
    run = next((k for k in range(1, len(late)) if late[k] != late[0] - k), len(late))

    def ways(ms):
        return [d for m in ms for d in (m, n - m)]

    at = iota((8, width), 1)
    code = (position(at) + 1).astype(F32).astype(BF16)
    slot_wide = iota((CAP, width), 0).astype(F32)
    slot = iota((CAP, BLOCK), 0).astype(F32)
    lane = iota((1, BLOCK), 1)

    def choose(c):
        chosen = hot(slot_wide == rank[pl.ds(c, 1), :])
        blocks = spec[:, pl.ds(c * PER, PER)].reshape(width, BLOCK)
        return jnp.dot(chosen, blocks, preferred_element_type=F32), dot_nt(code, chosen)[0:1]

    def build(c):
        power, codes = choose(c)
        normal = (power - mean[pl.ds(c, 1), :]) / sigma[pl.ds(c, 1), :]
        return jnp.where(slot < filled[pl.ds(c, 1), :], normal, 0.0).astype(BF16), codes

    def pack(d):
        payload, codes = build(source_of[(me + d) % n])
        send_rows[d] = payload
        send_codes[d] = codes

    def copies(send_buffer, buffer, sems):
        def copy(d):
            return pltpu.make_async_remote_copy(
                src_ref=send_buffer.at[d], dst_ref=buffer.at[me],
                send_sem=sems.at[0, d], recv_sem=sems.at[1, d],
                device_id={"freq": (me + d) % n}, device_id_type=MESH,
            )
        return copy

    row_copy = copies(send_rows, rows, row_sems)
    code_copy = copies(send_codes, got_codes, code_sems)
    norm_copy = copies(send_norms, got_norms, norm_sems)

    def send(d):
        code_copy(d).start()
        row_copy(d).start()

    def each_late(act):
        def body(k, carry):
            act(late[0] - k)
            act(n - late[0] + k)
            return carry
        act(far)
        if late:
            lax.fori_loop(0, run, body, 0)
        for d in ways(late[run:]):
            act(d)

    def tell(k):
        if k < rounds:
            for to in (me + REACH, me + n - REACH):
                pl.semaphore_signal(chain.at[k], inc=1, device_id={"freq": to % n}, device_id_type=MESH)

    def hear(k):
        if k < rounds:
            pl.semaphore_wait(chain.at[k], 2)
            tell(k + 1)

    owned = [owner[k] for k in range(coarse)]
    sources = []
    for d in ways(early):
        wanted, found = (me + d) % n * coarse + me, 0
        for k in range(coarse):
            found = jnp.where(owned[k] == wanted, k, found)
        sources.append(found)
    for copy in large:
        copy.wait()
    for d, c in zip(ways(early), sources):
        power, codes = choose(c)
        send_rows[d] = power.astype(BF16)
        send_codes[d] = codes
    pl.semaphore_wait(barrier, 2 * REACH + 1)
    tell(0)
    for d in ways(early):
        send(d)

    def stats(c, carry):
        center = BIN_STEP * median[c].astype(F32)
        deviation = mad[c].astype(F32)
        wide = MAD_WIDTH * BIN_STEP * deviation
        mean[pl.ds(c, 1), :] = jnp.full((1, BLOCK), center, F32)
        sigma[pl.ds(c, 1), :] = jnp.full((1, BLOCK), MAD_SCALE * BIN_STEP * deviation, F32)
        found = 0
        for k in range(coarse):
            found = jnp.where(owner[k] == c * coarse + me, k, found)
        source_of[c] = found
        x = spec[:, pl.ds(c * PER, PER)].astype(F32)
        inside = (x >= center - wide) & (x <= center + wide)
        kept = jnp.where(inside, x - center, 0.0)
        for k, each in enumerate((jnp.where(inside, 1.0, 0.0), kept, kept * kept)):
            mine[k, pl.ds(c, 1), :] = jnp.sum(jnp.sum(each, axis=(0, 1)), axis=0, keepdims=True)
        return carry

    lax.fori_loop(0, coarse, stats, 0, unroll=2)
    hear(0)
    share = pltpu.make_async_remote_copy(
        src_ref=mine, dst_ref=theirs, send_sem=stat_sems.at[0], recv_sem=stat_sems.at[1],
        device_id={"sub": 1 - half}, device_id_type=MESH,
    )
    share.start()
    share.wait()
    total = [jnp.sum(mine[k] + theirs[k], axis=1, keepdims=True) for k in range(3)]
    floor = jnp.maximum(total[0], 1.0)
    mean[...] = mean[...] + total[1] / floor
    sigma[...] = jnp.sqrt(0.5 * total[2] / floor + 0.5 * sigma[...] * sigma[...])
    for d, c in zip(ways(early), sources):
        send_norms[d] = jnp.where(lane < BLOCK // 2, mean[pl.ds(c, 1), :], sigma[pl.ds(c, 1), :])
    for d in ways(middle):
        pack(d)
    for d in ways(early):
        norm_copy(d).start()
    for d in ways(middle):
        send(d)
    hear(1)
    each_late(pack)
    for k in range(2, rounds):
        hear(k)
    each_late(lambda d: code_copy(d).start())
    each_late(lambda d: row_copy(d).start())

    ones = jnp.ones((8, BLOCK), BF16)

    def sender(d):
        return (me + n - d) % n

    def take_codes(s):
        codes = got_codes[s]
        base = (s * total_drift + half * drift) * PER - 1
        keys[pl.ds(s, 1), :] = jnp.where(codes > 0, codes + base.astype(F32), -1.0)

    def take_rows(s):
        over = jnp.maximum(rows[s].astype(F32) - THRESH, 0.0)
        coarse_part = over.astype(BF16)
        fine_part = (over - coarse_part.astype(F32)).astype(BF16)
        excess[pl.ds(s, 1), :] = (dot_nt(ones, coarse_part) + dot_nt(ones, fine_part))[0:1]

    def codes_in(d):
        code_copy(d).wait()
        take_codes(sender(d))

    def rows_in(d):
        row_copy(d).wait()
        take_rows(sender(d))

    payload, codes = build(source_of[me])
    rows[me] = payload
    got_codes[me] = codes
    take_codes(me)
    take_rows(me)
    for d in ways(early):
        s = sender(d)
        codes_in(d)
        row_copy(d).wait()
        norm_copy(d).wait()
        live = jnp.sum(jnp.where(got_codes[s] > 0, 1.0, 0.0), axis=1, keepdims=True)
        norms = got_norms[s]
        normal = (rows[s].astype(F32) - norms[:, 0:1]) / norms[:, BLOCK // 2 : BLOCK // 2 + 1]
        rows[s] = jnp.where(slot < live, normal, 0.0).astype(BF16)
        take_rows(s)
    for d in ways(middle):
        codes_in(d)
        rows_in(d)
    each_late(codes_in)
    counts = dot_nt(ones, hot(keys[...] >= 0))
    earlier = hot(iota((n, n), 0) < iota((n, n), 1))
    begins[...] = jnp.dot(counts.astype(BF16), earlier, preferred_element_type=F32).astype(jnp.int32)
    each_late(rows_in)


def compact_kernel(n, begins, rows, keys, excess, snr_out, keys_out, excess_out, wide, key_rows, excess_rows):
    wide[...] = jnp.zeros_like(wide)
    key_rows[...] = jnp.full_like(key_rows, -1.0)
    excess_rows[...] = jnp.zeros_like(excess_rows)
    lane = lax.broadcasted_iota(jnp.int32, (1, BLOCK), 1)
    for s in range(n):
        begin = begins[0, s]
        wide[pl.ds(begin, CAP), :] = rows[s].astype(F32)
        row, shift = begin // BLOCK, begin % BLOCK
        for source, target, empty in ((keys, key_rows, -1.0), (excess, excess_rows, 0.0)):
            turned = pltpu.roll(source[pl.ds(s, 1), :], shift, 1)
            here, after = pl.ds(row, 1), pl.ds(row + 1, 1)
            target[here, :] = jnp.where(lane >= shift, turned, target[here, :])
            target[after, :] = jnp.where(lane < shift, turned, empty)
    snr_out[...] = wide[...].astype(BF16)
    keys_out[...] = key_rows[0:n, :].astype(jnp.int32)
    excess_out[...] = excess_rows[0:n, :]


def per_device(spectrum, hit_mask, owner_map, median_bin, mad_bin):
    drift = spectrum.shape[0]
    coarse = owner_map.shape[0]
    n = lax.axis_size("freq")
    total_drift = drift * lax.axis_size("sub")
    width = PER * drift
    vmem, smem = pl.BlockSpec(memory_space=VMEM), pl.BlockSpec(memory_space=SMEM)
    tiles = spectrum.reshape(drift // 8, 8, coarse * PER, BLOCK).transpose(0, 2, 1, 3)
    table, line = VMEM((coarse, BLOCK), F32), VMEM((n, 1, CAP), F32)
    dma = pltpu.SemaphoreType.DMA
    rows, keys, excess, begins = pl.pallas_call(
        functools.partial(exchange_kernel, n, coarse, drift, total_drift),
        out_shape=[
            jax.ShapeDtypeStruct((n, CAP, BLOCK), BF16),
            jax.ShapeDtypeStruct((n, BLOCK), F32),
            jax.ShapeDtypeStruct((n, BLOCK), F32),
            jax.ShapeDtypeStruct((8, n), jnp.int32),
        ],
        in_specs=[pl.BlockSpec(memory_space=pltpu.HBM)] * 5,
        out_specs=[vmem] * 4,
        scratch_shapes=[
            SMEM((coarse,), jnp.int32), SMEM((coarse,), jnp.int32), SMEM((coarse,), jnp.int32),
            SMEM((coarse,), jnp.int32),
            VMEM(hit_mask.shape, jnp.int32), VMEM(tiles.shape, BF16),
            VMEM((3, coarse, BLOCK), F32), VMEM((3, coarse, BLOCK), F32), table, table,
            VMEM((coarse, width), F32), table,
            VMEM((n, CAP, BLOCK), BF16), line, line, line, line,
            dma((4,)), dma((4,)), dma((2,)), dma((2, n)), dma((2, n)), dma((2, n)),
            pltpu.SemaphoreType.REGULAR((max(n // 2 // REACH - 1, 1),)),
        ],
        compiler_params=pltpu.CompilerParams(
            collective_id=0, has_side_effects=True, vmem_limit_bytes=16 * 1024 * 1024
        ),
        name="exchange",
    )(*(pltpu.with_memory_space_constraint(x, pltpu.HBM) for x in (owner_map, median_bin, mad_bin, hit_mask, tiles)))
    snr, keys, excess = pl.pallas_call(
        functools.partial(compact_kernel, n),
        out_shape=[
            jax.ShapeDtypeStruct((n * CAP, BLOCK), BF16),
            jax.ShapeDtypeStruct((n, BLOCK), jnp.int32),
            jax.ShapeDtypeStruct((n, BLOCK), F32),
        ],
        in_specs=[smem] + [vmem] * 3,
        out_specs=[vmem] * 3,
        scratch_shapes=[VMEM((n * CAP, BLOCK), F32), VMEM((n + 8, BLOCK), F32), VMEM((n + 8, BLOCK), F32)],
        compiler_params=pltpu.CompilerParams(vmem_limit_bytes=16 * 1024 * 1024),
        name="compact",
    )(begins, rows, keys, excess)
    total = n * CAP
    return snr.reshape(1, 1, total, BLOCK), keys.reshape(1, 1, total), excess.reshape(1, 1, total)


def solution(mesh):
    placed = (
        P("sub", ("beam", "freq")),
        P("sub", ("beam", "freq")),
        P(("beam", "freq")),
        P(("beam", "freq")),
        P(("beam", "freq")),
    )
    return jax.shard_map(
        per_device,
        mesh=mesh,
        in_specs=placed,
        out_specs=(
            P("freq", "sub", "beam", None),
            P("freq", "sub", "beam"),
            P("freq", "sub", "beam"),
        ),
        check_vma=False,
    )
```

```python
import functools

import jax
import jax.numpy as jnp
from jax import lax
from jax.experimental import pallas as pl
from jax.experimental.pallas import tpu as pltpu
from jax.sharding import PartitionSpec as P

COARSE_WIDTH = 1024
BLOCK = 128
CAP = 128
PER = COARSE_WIDTH // BLOCK

BIN_STEP = 0.0625
MAD_WIDTH = 5.0
MAD_SCALE = 1.4826
THRESH = 3.0

VMEM = pltpu.VMEM
SMEM = pltpu.SMEM
MESH = pl.DeviceIdType.MESH
F32 = jnp.float32
BF16 = jnp.bfloat16


def dot_nt(a, b):
    return lax.dot_general(a, b, (((1,), (1,)), ((), ())), preferred_element_type=F32)


REACH = 2


def exchange_kernel(
    n, coarse, drift, total_drift,
    owner_hbm, median_hbm, mad_hbm, marks_hbm, spec_hbm,
    rows, keys, excess, begins,
    owner, median, mad, source_of, marks, spec, mine, theirs, mean, sigma, rank, filled,
    send_rows, send_codes, got_codes, send_norms, got_norms,
    small_sems, spec_sems, stat_sems, row_sems, code_sems, norm_sems, chain,
):
    me = lax.axis_index("freq")
    half = lax.axis_index("sub")
    far = n // 2
    rounds = far // REACH - 1
    groups = spec_sems.shape[0]
    group = coarse // groups
    width = PER * drift
    barrier = pltpu.get_barrier_semaphore()
    small = [
        pltpu.make_async_copy(src, dst, small_sems.at[k])
        for k, (src, dst) in enumerate(
            ((owner_hbm, owner), (median_hbm, median), (mad_hbm, mad), (marks_hbm, marks))
        )
    ]
    large = []
    for g in range(groups):
        part = pl.ds(g * group * PER, group * PER)
        large.append(pltpu.make_async_copy(spec_hbm.at[:, part], spec.at[:, part], spec_sems.at[g]))
    for copy in small + large:
        copy.start()
    for d in range(REACH, 0, -1):
        for to in (me + d, me + n - d):
            pl.semaphore_signal(barrier, inc=1, device_id={"freq": to % n}, device_id_type=MESH)
    pl.semaphore_signal(barrier, inc=1, device_id={"sub": 1 - half}, device_id_type=MESH)

    for copy in small:
        copy.wait()

    def position(at):
        tile, block, row = at // (PER * 8), at // 8 % PER, at % 8
        return (tile * 8 + row) * PER + block

    def iota(shape, axis):
        return lax.broadcasted_iota(jnp.int32, shape, axis)

    def hot(mask):
        return jnp.where(mask, 1.0, 0.0).astype(BF16)

    lanes = coarse * PER
    spread = hot(iota((lanes, lanes), 1) == iota((lanes, lanes), 0) % coarse * PER + iota((lanes, lanes), 0) // coarse)
    by_block = dot_nt(spread, marks[...].astype(F32).astype(BF16)).astype(BF16)
    ranks = set_here = None
    for b in range(PER):
        here = by_block[b * coarse : (b + 1) * coarse]
        come, go = iota((drift, width), 0) * PER + b, position(iota((drift, width), 1))
        before = jnp.dot(here, hot(come < go), preferred_element_type=F32)
        same = jnp.dot(here, hot(come == go), preferred_element_type=F32)
        ranks = before if b == 0 else ranks + before
        set_here = same if b == 0 else set_here + same
    rank[...] = jnp.where(set_here > 0, ranks, -1.0)
    filled[...] = jnp.broadcast_to(jnp.sum(set_here, axis=1, keepdims=True), filled.shape)

    early = [m for m in (2, 1, 4, 3) if m <= 2 * REACH and m < far]
    middle = [m for m in (6, 5) if 2 * REACH < m <= 3 * REACH and m < far]
    late = [m for m in range(far - 1, 0, -1) if m not in early + middle]

    def ways(ms):
        return [d for m in ms for d in (m, n - m)]

    at = iota((8, width), 1)
    code = (position(at) + 1).astype(F32).astype(BF16)
    slot_wide = iota((CAP, width), 0).astype(F32)
    slot = iota((CAP, BLOCK), 0).astype(F32)
    lane = iota((1, BLOCK), 1)

    def choose(c):
        chosen = hot(slot_wide == rank[pl.ds(c, 1), :])
        blocks = spec[:, pl.ds(c * PER, PER)].reshape(width, BLOCK)
        return jnp.dot(chosen, blocks, preferred_element_type=F32), dot_nt(code, chosen)[0:1]

    def build(c):
        power, codes = choose(c)
        normal = (power - mean[pl.ds(c, 1), :]) / sigma[pl.ds(c, 1), :]
        return jnp.where(slot < filled[pl.ds(c, 1), :], normal, 0.0).astype(BF16), codes

    def pack(d):
        payload, codes = build(source_of[(me + d) % n])
        send_rows[d] = payload
        send_codes[d] = codes

    def copies(send_buffer, buffer, sems):
        def copy(d):
            return pltpu.make_async_remote_copy(
                src_ref=send_buffer.at[d], dst_ref=buffer.at[me],
                send_sem=sems.at[0, d], recv_sem=sems.at[1, d],
                device_id={"freq": (me + d) % n}, device_id_type=MESH,
            )
        return copy

    row_copy = copies(send_rows, rows, row_sems)
    code_copy = copies(send_codes, got_codes, code_sems)
    norm_copy = copies(send_norms, got_norms, norm_sems)

    def send(d):
        code_copy(d).start()
        row_copy(d).start()

    def each_late(act):
        act(far)
        at = 0
        while at < len(late):
            size = next((k for k in range(1, len(late) - at) if late[at + k] != late[at] - k), len(late) - at)
            if size > 2:
                def body(k, carry, top=late[at]):
                    act(top - k)
                    act(n - top + k)
                    return carry
                lax.fori_loop(0, size, body, 0)
            else:
                for d in ways(late[at : at + size]):
                    act(d)
            at += size

    def tell(k):
        if k < rounds:
            for to in (me + REACH, me + n - REACH):
                pl.semaphore_signal(chain.at[k], inc=1, device_id={"freq": to % n}, device_id_type=MESH)

    def hear(k):
        if k < rounds:
            pl.semaphore_wait(chain.at[k], 2)
            tell(k + 1)

    owned = [owner[k] for k in range(coarse)]
    sources = []
    for d in ways(early):
        wanted, found = (me + d) % n * coarse + me, 0
        for k in range(coarse):
            found = jnp.where(owned[k] == wanted, k, found)
        sources.append(found)
    for copy in large:
        copy.wait()
    for d, c in zip(ways(early), sources):
        power, codes = choose(c)
        send_rows[d] = power.astype(BF16)
        send_codes[d] = codes
    pl.semaphore_wait(barrier, 2 * REACH + 1)
    tell(0)
    for d in ways([m for m in early if m <= REACH]):
        send(d)
    hear(0)
    for d in ways([m for m in early if m > REACH]):
        send(d)

    def stats(c, carry):
        center = BIN_STEP * median[c].astype(F32)
        deviation = mad[c].astype(F32)
        wide = MAD_WIDTH * BIN_STEP * deviation
        mean[pl.ds(c, 1), :] = jnp.full((1, BLOCK), center, F32)
        sigma[pl.ds(c, 1), :] = jnp.full((1, BLOCK), MAD_SCALE * BIN_STEP * deviation, F32)
        found = 0
        for k in range(coarse):
            found = jnp.where(owner[k] == c * coarse + me, k, found)
        source_of[c] = found
        x = spec[:, pl.ds(c * PER, PER)].astype(F32)
        inside = (x >= center - wide) & (x <= center + wide)
        kept = jnp.where(inside, x - center, 0.0)
        for k, each in enumerate((jnp.where(inside, 1.0, 0.0), kept, kept * kept)):
            mine[k, pl.ds(c, 1), :] = jnp.sum(jnp.sum(each, axis=(0, 1)), axis=0, keepdims=True)
        return carry

    lax.fori_loop(0, coarse // 2, stats, 0, unroll=2)
    hear(1)
    lax.fori_loop(coarse // 2, coarse, stats, 0, unroll=2)
    hear(2)
    share = pltpu.make_async_remote_copy(
        src_ref=mine, dst_ref=theirs, send_sem=stat_sems.at[0], recv_sem=stat_sems.at[1],
        device_id={"sub": 1 - half}, device_id_type=MESH,
    )
    share.start()
    share.wait()
    hear(3)
    total = [jnp.sum(mine[k] + theirs[k], axis=1, keepdims=True) for k in range(3)]
    floor = jnp.maximum(total[0], 1.0)
    mean[...] = mean[...] + total[1] / floor
    sigma[...] = jnp.sqrt(0.5 * total[2] / floor + 0.5 * sigma[...] * sigma[...])
    for d, c in zip(ways(early), sources):
        send_norms[d] = jnp.where(lane < BLOCK // 2, mean[pl.ds(c, 1), :], sigma[pl.ds(c, 1), :])
    for d in ways(middle):
        pack(d)
    for d in ways(early):
        norm_copy(d).start()
    for d in ways(middle):
        send(d)
    hear(4)
    each_late(pack)
    for k in range(5, rounds):
        hear(k)
    each_late(lambda d: code_copy(d).start())
    each_late(lambda d: row_copy(d).start())

    ones = jnp.ones((8, BLOCK), BF16)

    def sender(d):
        return (me + n - d) % n

    def take_codes(s):
        codes = got_codes[s]
        base = (s * total_drift + half * drift) * PER - 1
        keys[pl.ds(s, 1), :] = jnp.where(codes > 0, codes + base.astype(F32), -1.0)

    def take_rows(s):
        over = jnp.maximum(rows[s].astype(F32) - THRESH, 0.0)
        coarse_part = over.astype(BF16)
        fine_part = (over - coarse_part.astype(F32)).astype(BF16)
        excess[pl.ds(s, 1), :] = (dot_nt(ones, coarse_part) + dot_nt(ones, fine_part))[0:1]

    def codes_in(d):
        code_copy(d).wait()
        take_codes(sender(d))

    def rows_in(d):
        row_copy(d).wait()
        take_rows(sender(d))

    payload, codes = build(source_of[me])
    rows[me] = payload
    got_codes[me] = codes
    take_codes(me)
    take_rows(me)
    for d in ways(early):
        s = sender(d)
        codes_in(d)
        row_copy(d).wait()
        norm_copy(d).wait()
        live = jnp.sum(jnp.where(got_codes[s] > 0, 1.0, 0.0), axis=1, keepdims=True)
        norms = got_norms[s]
        normal = (rows[s].astype(F32) - norms[:, 0:1]) / norms[:, BLOCK // 2 : BLOCK // 2 + 1]
        rows[s] = jnp.where(slot < live, normal, 0.0).astype(BF16)
        take_rows(s)
    for d in ways(middle):
        codes_in(d)
        rows_in(d)
    each_late(codes_in)
    counts = dot_nt(ones, hot(keys[...] >= 0))
    earlier = hot(iota((n, n), 0) < iota((n, n), 1))
    begins[...] = jnp.dot(counts.astype(BF16), earlier, preferred_element_type=F32).astype(jnp.int32)
    each_late(rows_in)


def compact_kernel(
    n, begins_vmem, rows, keys, excess, snr_out, keys_out, excess_out, wide, narrow, key_rows, excess_rows, begins, sems
):
    fetch = pltpu.make_async_copy(begins_vmem, begins, sems.at[0])
    fetch.start()
    wide[...] = jnp.zeros_like(wide)
    key_rows[...] = jnp.full_like(key_rows, -1.0)
    excess_rows[...] = jnp.zeros_like(excess_rows)
    lane = lax.broadcasted_iota(jnp.int32, (1, BLOCK), 1)
    fetch.wait()
    for s in range(n):
        wide[pl.ds(begins[0, s], CAP), :] = rows[s].astype(F32)
    parts = sems.shape[0] - 1
    size = n * CAP // parts
    writes = []
    for k in range(parts):
        part = pl.ds(k * size, size)
        narrow[part, :] = wide[part, :].astype(BF16)
        writes.append(pltpu.make_async_copy(narrow.at[part, :], snr_out.at[part, :], sems.at[k + 1]))
        if k:
            writes[k - 1].start()
    for s in range(n):
        row, shift = lax.div(begins[0, s], BLOCK), lax.rem(begins[0, s], BLOCK)
        for source, target, empty in ((keys, key_rows, -1.0), (excess, excess_rows, 0.0)):
            turned = pltpu.roll(source[pl.ds(s, 1), :], shift, 1)
            here, after = pl.ds(row, 1), pl.ds(row + 1, 1)
            target[here, :] = jnp.where(lane >= shift, turned, target[here, :])
            target[after, :] = jnp.where(lane < shift, turned, empty)
        if s == 0:
            writes[-1].start()
    keys_out[...] = key_rows[0:n, :].astype(jnp.int32)
    excess_out[...] = excess_rows[0:n, :]
    for write in writes:
        write.wait()


def per_device(spectrum, hit_mask, owner_map, median_bin, mad_bin):
    drift = spectrum.shape[0]
    coarse = owner_map.shape[0]
    n = lax.axis_size("freq")
    total_drift = drift * lax.axis_size("sub")
    width = PER * drift
    vmem = pl.BlockSpec(memory_space=VMEM)
    tiles = spectrum.reshape(drift // 8, 8, coarse * PER, BLOCK).transpose(0, 2, 1, 3)
    table, line = VMEM((coarse, BLOCK), F32), VMEM((n, 1, CAP), F32)
    dma = pltpu.SemaphoreType.DMA
    rows, keys, excess, begins = pl.pallas_call(
        functools.partial(exchange_kernel, n, coarse, drift, total_drift),
        out_shape=[
            jax.ShapeDtypeStruct((n, CAP, BLOCK), BF16),
            jax.ShapeDtypeStruct((n, BLOCK), F32),
            jax.ShapeDtypeStruct((n, BLOCK), F32),
            jax.ShapeDtypeStruct((8, n), jnp.int32),
        ],
        in_specs=[pl.BlockSpec(memory_space=pltpu.HBM)] * 5,
        out_specs=[vmem] * 4,
        scratch_shapes=[
            SMEM((coarse,), jnp.int32), SMEM((coarse,), jnp.int32), SMEM((coarse,), jnp.int32),
            SMEM((coarse,), jnp.int32),
            VMEM(hit_mask.shape, jnp.int32), VMEM(tiles.shape, BF16),
            VMEM((3, coarse, BLOCK), F32), VMEM((3, coarse, BLOCK), F32), table, table,
            VMEM((coarse, width), F32), table,
            VMEM((n, CAP, BLOCK), BF16), line, line, line, line,
            dma((4,)), dma((4,)), dma((2,)), dma((2, n)), dma((2, n)), dma((2, n)),
            pltpu.SemaphoreType.REGULAR((max(n // 2 // REACH - 1, 1),)),
        ],
        compiler_params=pltpu.CompilerParams(
            collective_id=0, has_side_effects=True, vmem_limit_bytes=16 * 1024 * 1024
        ),
        name="exchange",
    )(*(pltpu.with_memory_space_constraint(x, pltpu.HBM) for x in (owner_map, median_bin, mad_bin, hit_mask, tiles)))
    snr, keys, excess = pl.pallas_call(
        functools.partial(compact_kernel, n),
        out_shape=[
            jax.ShapeDtypeStruct((n * CAP, BLOCK), BF16),
            jax.ShapeDtypeStruct((n, BLOCK), jnp.int32),
            jax.ShapeDtypeStruct((n, BLOCK), F32),
        ],
        in_specs=[vmem] * 4,
        out_specs=[pl.BlockSpec(memory_space=pltpu.HBM), vmem, vmem],
        scratch_shapes=[
            VMEM((n * CAP, BLOCK), F32), VMEM((n * CAP, BLOCK), BF16),
            VMEM((n + 8, BLOCK), F32), VMEM((n + 8, BLOCK), F32), SMEM((8, n), jnp.int32), dma((5,)),
        ],
        compiler_params=pltpu.CompilerParams(vmem_limit_bytes=16 * 1024 * 1024),
        name="compact",
    )(begins, rows, keys, excess)
    total = n * CAP
    return snr.reshape(1, 1, total, BLOCK), keys.reshape(1, 1, total), excess.reshape(1, 1, total)


def solution(mesh):
    placed = (
        P("sub", ("beam", "freq")),
        P("sub", ("beam", "freq")),
        P(("beam", "freq")),
        P(("beam", "freq")),
        P(("beam", "freq")),
    )
    return jax.shard_map(
        per_device,
        mesh=mesh,
        in_specs=placed,
        out_specs=(
            P("freq", "sub", "beam", None),
            P("freq", "sub", "beam"),
            P("freq", "sub", "beam"),
        ),
        check_vma=False,
    )
```

```python
import functools

import jax
import jax.numpy as jnp
from jax import lax
from jax.experimental import pallas as pl
from jax.experimental.pallas import tpu as pltpu
from jax.sharding import PartitionSpec as P

COARSE_WIDTH = 1024
BLOCK = 128
CAP = 128
PER = COARSE_WIDTH // BLOCK

BIN_STEP = 0.0625
MAD_WIDTH = 5.0
MAD_SCALE = 1.4826
THRESH = 3.0

VMEM = pltpu.VMEM
SMEM = pltpu.SMEM
MESH = pl.DeviceIdType.MESH
F32 = jnp.float32
BF16 = jnp.bfloat16


def dot_nt(a, b):
    return lax.dot_general(a, b, (((1,), (1,)), ((), ())), preferred_element_type=F32)


REACH = 4


def exchange_kernel(
    n, coarse, drift, total_drift,
    owner_hbm, median_hbm, mad_hbm, marks_hbm, spec_hbm,
    rows, keys, excess, begins,
    owner, median, mad, source_of, marks, spec, mine, theirs, mean, sigma, rank, filled,
    send_rows, send_codes, got_codes, send_norms, got_norms,
    small_sems, spec_sems, stat_sems, row_sems, code_sems, norm_sems, chain,
):
    me = lax.axis_index("freq")
    half = lax.axis_index("sub")
    far = n // 2
    rounds = far // REACH - 1
    groups = spec_sems.shape[0]
    group = coarse // groups
    width = PER * drift
    barrier = pltpu.get_barrier_semaphore()
    small = [
        pltpu.make_async_copy(src, dst, small_sems.at[k])
        for k, (src, dst) in enumerate(
            ((owner_hbm, owner), (median_hbm, median), (mad_hbm, mad), (marks_hbm, marks))
        )
    ]
    large = []
    for g in range(groups):
        part = pl.ds(g * group * PER, group * PER)
        large.append(pltpu.make_async_copy(spec_hbm.at[:, part], spec.at[:, part], spec_sems.at[g]))
    for copy in small + large:
        copy.start()
    pl.semaphore_signal(barrier, inc=1, device_id={"sub": 1 - half}, device_id_type=MESH)
    for d in range(1, REACH + 1):
        for to in (me + d, me + n - d):
            pl.semaphore_signal(barrier, inc=1, device_id={"freq": to % n}, device_id_type=MESH)

    for copy in small:
        copy.wait()

    def position(at):
        tile, block, row = at // (PER * 8), at // 8 % PER, at % 8
        return (tile * 8 + row) * PER + block

    def iota(shape, axis):
        return lax.broadcasted_iota(jnp.int32, shape, axis)

    def hot(mask):
        return jnp.where(mask, 1.0, 0.0).astype(BF16)

    lanes = coarse * PER
    spread = hot(iota((lanes, lanes), 1) == iota((lanes, lanes), 0) % coarse * PER + iota((lanes, lanes), 0) // coarse)
    by_block = dot_nt(spread, marks[...].astype(F32).astype(BF16)).astype(BF16)
    ranks = set_here = None
    for b in range(PER):
        here = by_block[b * coarse : (b + 1) * coarse]
        come, go = iota((drift, width), 0) * PER + b, position(iota((drift, width), 1))
        before = jnp.dot(here, hot(come < go), preferred_element_type=F32)
        same = jnp.dot(here, hot(come == go), preferred_element_type=F32)
        ranks = before if b == 0 else ranks + before
        set_here = same if b == 0 else set_here + same
    rank[...] = jnp.where(set_here > 0, ranks, -1.0)
    filled[...] = jnp.broadcast_to(jnp.sum(set_here, axis=1, keepdims=True), filled.shape)

    early = [m for m in (4, 3, 2, 1) if m <= REACH and m < far]
    middle = [m for m in (6, 5) if REACH < m <= 2 * REACH and m < far]
    late = [m for m in range(far - 1, 0, -1) if m not in early + middle]

    def ways(ms):
        return [d for m in ms for d in (m, n - m)]

    at = iota((8, width), 1)
    code = (position(at) + 1).astype(F32).astype(BF16)
    slot_wide = iota((CAP, width), 0).astype(F32)
    slot = iota((CAP, BLOCK), 0).astype(F32)
    lane = iota((1, BLOCK), 1)

    def choose(c):
        chosen = hot(slot_wide == rank[pl.ds(c, 1), :])
        blocks = spec[:, pl.ds(c * PER, PER)].reshape(width, BLOCK)
        return jnp.dot(chosen, blocks, preferred_element_type=F32), dot_nt(code, chosen)[0:1]

    def build(c):
        power, codes = choose(c)
        normal = (power - mean[pl.ds(c, 1), :]) / sigma[pl.ds(c, 1), :]
        return jnp.where(slot < filled[pl.ds(c, 1), :], normal, 0.0).astype(BF16), codes

    def pack(d):
        payload, codes = build(source_of[(me + d) % n])
        send_rows[d] = payload
        send_codes[d] = codes

    def copies(send_buffer, buffer, sems):
        def copy(d):
            return pltpu.make_async_remote_copy(
                src_ref=send_buffer.at[d], dst_ref=buffer.at[me],
                send_sem=sems.at[0, d], recv_sem=sems.at[1, d],
                device_id={"freq": (me + d) % n}, device_id_type=MESH,
            )
        return copy

    row_copy = copies(send_rows, rows, row_sems)
    code_copy = copies(send_codes, got_codes, code_sems)
    norm_copy = copies(send_norms, got_norms, norm_sems)

    def send(d):
        code_copy(d).start()
        row_copy(d).start()

    def each_late(act):
        act(far)
        at = 0
        while at < len(late):
            size = next((k for k in range(1, len(late) - at) if late[at + k] != late[at] - k), len(late) - at)
            if size > 2:
                def body(k, carry, top=late[at]):
                    act(top - k)
                    act(n - top + k)
                    return carry
                lax.fori_loop(0, size, body, 0)
            else:
                for d in ways(late[at : at + size]):
                    act(d)
            at += size

    def tell(k):
        if k < rounds:
            for to in (me + REACH, me + n - REACH):
                pl.semaphore_signal(chain.at[k], inc=1, device_id={"freq": to % n}, device_id_type=MESH)

    def hear(k):
        if k < rounds:
            pl.semaphore_wait(chain.at[k], 2)
            tell(k + 1)

    owned = [owner[k] for k in range(coarse)]
    sources = []
    for d in ways(early):
        wanted, found = (me + d) % n * coarse + me, 0
        for k in range(coarse):
            found = jnp.where(owned[k] == wanted, k, found)
        sources.append(found)
    for copy in large:
        copy.wait()
    for d, c in zip(ways(early), sources):
        power, codes = choose(c)
        send_rows[d] = power.astype(BF16)
        send_codes[d] = codes
    pl.semaphore_wait(barrier, 2 * REACH + 1)
    tell(0)
    for d in ways(early):
        send(d)

    def stats(c, carry):
        center = BIN_STEP * median[c].astype(F32)
        deviation = mad[c].astype(F32)
        wide = MAD_WIDTH * BIN_STEP * deviation
        mean[pl.ds(c, 1), :] = jnp.full((1, BLOCK), center, F32)
        sigma[pl.ds(c, 1), :] = jnp.full((1, BLOCK), MAD_SCALE * BIN_STEP * deviation, F32)
        found = 0
        for k in range(coarse):
            found = jnp.where(owner[k] == c * coarse + me, k, found)
        source_of[c] = found
        x = spec[:, pl.ds(c * PER, PER)].astype(F32)
        inside = (x >= center - wide) & (x <= center + wide)
        kept = jnp.where(inside, x - center, 0.0)
        for k, each in enumerate((jnp.where(inside, 1.0, 0.0), kept, kept * kept)):
            mine[k, pl.ds(c, 1), :] = jnp.sum(jnp.sum(each, axis=(0, 1)), axis=0, keepdims=True)
        return carry

    lax.fori_loop(0, coarse, stats, 0, unroll=2)
    hear(0)
    share = pltpu.make_async_remote_copy(
        src_ref=mine, dst_ref=theirs, send_sem=stat_sems.at[0], recv_sem=stat_sems.at[1],
        device_id={"sub": 1 - half}, device_id_type=MESH,
    )
    share.start()
    share.wait()
    total = [jnp.sum(mine[k] + theirs[k], axis=1, keepdims=True) for k in range(3)]
    floor = jnp.maximum(total[0], 1.0)
    mean[...] = mean[...] + total[1] / floor
    sigma[...] = jnp.sqrt(0.5 * total[2] / floor + 0.5 * sigma[...] * sigma[...])
    for d, c in zip(ways(early), sources):
        send_norms[d] = jnp.where(lane < BLOCK // 2, mean[pl.ds(c, 1), :], sigma[pl.ds(c, 1), :])
    for d in ways(middle):
        pack(d)
    for d in ways(early):
        norm_copy(d).start()
    for d in ways(middle):
        send(d)
    hear(1)
    each_late(pack)
    for k in range(2, rounds):
        hear(k)
    each_late(lambda d: code_copy(d).start())
    each_late(lambda d: row_copy(d).start())

    ones = jnp.ones((8, BLOCK), BF16)

    def sender(d):
        return (me + n - d) % n

    def take_codes(s):
        codes = got_codes[s]
        base = (s * total_drift + half * drift) * PER - 1
        keys[pl.ds(s, 1), :] = jnp.where(codes > 0, codes + base.astype(F32), -1.0)

    def take_rows(s):
        over = jnp.maximum(rows[s].astype(F32) - THRESH, 0.0)
        coarse_part = over.astype(BF16)
        fine_part = (over - coarse_part.astype(F32)).astype(BF16)
        excess[pl.ds(s, 1), :] = (dot_nt(ones, coarse_part) + dot_nt(ones, fine_part))[0:1]

    def codes_in(d):
        code_copy(d).wait()
        take_codes(sender(d))

    def rows_in(d):
        row_copy(d).wait()
        take_rows(sender(d))

    payload, codes = build(source_of[me])
    rows[me] = payload
    got_codes[me] = codes
    take_codes(me)
    take_rows(me)
    for d in ways(early):
        s = sender(d)
        codes_in(d)
        row_copy(d).wait()
        norm_copy(d).wait()
        live = jnp.sum(jnp.where(got_codes[s] > 0, 1.0, 0.0), axis=1, keepdims=True)
        norms = got_norms[s]
        normal = (rows[s].astype(F32) - norms[:, 0:1]) / norms[:, BLOCK // 2 : BLOCK // 2 + 1]
        rows[s] = jnp.where(slot < live, normal, 0.0).astype(BF16)
        take_rows(s)
    for d in ways(middle):
        codes_in(d)
        rows_in(d)
    each_late(codes_in)
    counts = dot_nt(ones, hot(keys[...] >= 0))
    earlier = hot(iota((n, n), 0) < iota((n, n), 1))
    begins[...] = jnp.dot(counts.astype(BF16), earlier, preferred_element_type=F32).astype(jnp.int32)
    each_late(rows_in)


def compact_kernel(
    n, begins_vmem, rows, keys, excess, snr_out, keys_out, excess_out, wide, narrow, key_rows, excess_rows, key_ints, begins, sems
):
    fetch = pltpu.make_async_copy(begins_vmem, begins, sems.at[0])
    fetch.start()
    wide[...] = jnp.zeros_like(wide)
    key_rows[...] = jnp.full_like(key_rows, -1.0)
    excess_rows[...] = jnp.zeros_like(excess_rows)
    lane = lax.broadcasted_iota(jnp.int32, (1, BLOCK), 1)
    fetch.wait()
    for s in range(n):
        begin = begins[0, s]
        wide[pl.ds(begin, CAP), :] = rows[s].astype(F32)
        row, shift = lax.div(begin, BLOCK), lax.rem(begin, BLOCK)
        for source, target, empty in ((keys, key_rows, -1.0), (excess, excess_rows, 0.0)):
            turned = pltpu.roll(source[pl.ds(s, 1), :], shift, 1)
            here, after = pl.ds(row, 1), pl.ds(row + 1, 1)
            target[here, :] = jnp.where(lane >= shift, turned, target[here, :])
            target[after, :] = jnp.where(lane < shift, turned, empty)
    key_ints[...] = key_rows[0:n, :].astype(jnp.int32)
    parts = sems.shape[0] - 3
    size = n * CAP // parts
    writes = [
        pltpu.make_async_copy(key_ints, keys_out, sems.at[parts + 1]),
        pltpu.make_async_copy(excess_rows.at[pl.ds(0, n), :], excess_out, sems.at[parts + 2]),
    ]
    for k in range(parts):
        part = pl.ds(k * size, size)
        narrow[part, :] = wide[part, :].astype(BF16)
        writes.append(pltpu.make_async_copy(narrow.at[part, :], snr_out.at[part, :], sems.at[k + 1]))
        if k == 1:
            writes[0].start()
            writes[1].start()
        if k:
            writes[k + 1].start()
    writes[-1].start()
    for write in writes:
        write.wait()


def per_device(spectrum, hit_mask, owner_map, median_bin, mad_bin):
    drift = spectrum.shape[0]
    coarse = owner_map.shape[0]
    n = lax.axis_size("freq")
    total_drift = drift * lax.axis_size("sub")
    width = PER * drift
    vmem = pl.BlockSpec(memory_space=VMEM)
    tiles = spectrum.reshape(drift // 8, 8, coarse * PER, BLOCK).transpose(0, 2, 1, 3)
    table, line = VMEM((coarse, BLOCK), F32), VMEM((n, 1, CAP), F32)
    dma = pltpu.SemaphoreType.DMA
    rows, keys, excess, begins = pl.pallas_call(
        functools.partial(exchange_kernel, n, coarse, drift, total_drift),
        out_shape=[
            jax.ShapeDtypeStruct((n, CAP, BLOCK), BF16),
            jax.ShapeDtypeStruct((n, BLOCK), F32),
            jax.ShapeDtypeStruct((n, BLOCK), F32),
            jax.ShapeDtypeStruct((8, n), jnp.int32),
        ],
        in_specs=[pl.BlockSpec(memory_space=pltpu.HBM)] * 5,
        out_specs=[vmem] * 4,
        scratch_shapes=[
            SMEM((coarse,), jnp.int32), SMEM((coarse,), jnp.int32), SMEM((coarse,), jnp.int32),
            SMEM((coarse,), jnp.int32),
            VMEM(hit_mask.shape, jnp.int32), VMEM(tiles.shape, BF16),
            VMEM((3, coarse, BLOCK), F32), VMEM((3, coarse, BLOCK), F32), table, table,
            VMEM((coarse, width), F32), table,
            VMEM((n, CAP, BLOCK), BF16), line, line, line, line,
            dma((4,)), dma((4,)), dma((2,)), dma((2, n)), dma((2, n)), dma((2, n)),
            pltpu.SemaphoreType.REGULAR((max(n // 2 // REACH - 1, 1),)),
        ],
        compiler_params=pltpu.CompilerParams(
            collective_id=0, has_side_effects=True, vmem_limit_bytes=16 * 1024 * 1024
        ),
        name="exchange",
    )(*(pltpu.with_memory_space_constraint(x, pltpu.HBM) for x in (owner_map, median_bin, mad_bin, hit_mask, tiles)))
    snr, keys, excess = pl.pallas_call(
        functools.partial(compact_kernel, n),
        out_shape=[
            jax.ShapeDtypeStruct((n * CAP, BLOCK), BF16),
            jax.ShapeDtypeStruct((n, BLOCK), jnp.int32),
            jax.ShapeDtypeStruct((n, BLOCK), F32),
        ],
        in_specs=[vmem] * 4,
        out_specs=[pl.BlockSpec(memory_space=pltpu.HBM)] * 3,
        scratch_shapes=[
            VMEM((n * CAP, BLOCK), F32), VMEM((n * CAP, BLOCK), BF16),
            VMEM((n + 8, BLOCK), F32), VMEM((n + 8, BLOCK), F32), VMEM((n, BLOCK), jnp.int32),
            SMEM((8, n), jnp.int32), dma((7,)),
        ],
        compiler_params=pltpu.CompilerParams(vmem_limit_bytes=16 * 1024 * 1024),
        name="compact",
    )(begins, rows, keys, excess)
    total = n * CAP
    return snr.reshape(1, 1, total, BLOCK), keys.reshape(1, 1, total), excess.reshape(1, 1, total)


def solution(mesh):
    placed = (
        P("sub", ("beam", "freq")),
        P("sub", ("beam", "freq")),
        P(("beam", "freq")),
        P(("beam", "freq")),
        P(("beam", "freq")),
    )
    return jax.shard_map(
        per_device,
        mesh=mesh,
        in_specs=placed,
        out_specs=(
            P("freq", "sub", "beam", None),
            P("freq", "sub", "beam"),
            P("freq", "sub", "beam"),
        ),
        check_vma=False,
    )
```

```python
import functools

import jax
import jax.numpy as jnp
from jax import lax
from jax.experimental import pallas as pl
from jax.experimental.pallas import tpu as pltpu
from jax.sharding import PartitionSpec as P

COARSE_WIDTH = 1024
BLOCK = 128
CAP = 128
PER = COARSE_WIDTH // BLOCK

BIN_STEP = 0.0625
MAD_WIDTH = 5.0
MAD_SCALE = 1.4826
THRESH = 3.0

VMEM = pltpu.VMEM
SMEM = pltpu.SMEM
MESH = pl.DeviceIdType.MESH
F32 = jnp.float32
BF16 = jnp.bfloat16


def dot_nt(a, b):
    return lax.dot_general(a, b, (((1,), (1,)), ((), ())), preferred_element_type=F32)


REACH = 4


def exchange_kernel(
    n, coarse, drift, total_drift,
    owner_hbm, median_hbm, mad_hbm, marks_hbm, spec_hbm,
    rows, keys, excess, begins,
    owner, median, mad, source_of, marks, spec, mine, theirs, mean, sigma, rank, filled,
    send_rows, send_codes, got_codes, send_norms, got_norms,
    small_sems, spec_sems, stat_sems, row_sems, code_sems, norm_sems, chain,
):
    me = lax.axis_index("freq")
    half = lax.axis_index("sub")
    far = n // 2
    rounds = far // REACH - 1
    groups = spec_sems.shape[0]
    group = coarse // groups
    width = PER * drift
    barrier = pltpu.get_barrier_semaphore()
    small = [
        pltpu.make_async_copy(src, dst, small_sems.at[k])
        for k, (src, dst) in enumerate(
            ((owner_hbm, owner), (median_hbm, median), (mad_hbm, mad), (marks_hbm, marks))
        )
    ]
    large = []
    for g in range(groups):
        part = pl.ds(g * group * PER, group * PER)
        large.append(pltpu.make_async_copy(spec_hbm.at[:, part], spec.at[:, part], spec_sems.at[g]))
    for copy in small + large:
        copy.start()
    pl.semaphore_signal(barrier, inc=1, device_id={"sub": 1 - half}, device_id_type=MESH)
    for d in range(1, REACH + 1):
        for to in (me + d, me + n - d):
            pl.semaphore_signal(barrier, inc=1, device_id={"freq": to % n}, device_id_type=MESH)

    for copy in small:
        copy.wait()

    def position(at):
        tile, block, row = at // (PER * 8), at // 8 % PER, at % 8
        return (tile * 8 + row) * PER + block

    def iota(shape, axis):
        return lax.broadcasted_iota(jnp.int32, shape, axis)

    def hot(mask):
        return jnp.where(mask, 1.0, 0.0).astype(BF16)

    lanes = coarse * PER
    spread = hot(iota((lanes, lanes), 1) == iota((lanes, lanes), 0) % coarse * PER + iota((lanes, lanes), 0) // coarse)
    by_block = dot_nt(spread, marks[...].astype(F32).astype(BF16)).astype(BF16)
    ranks = set_here = None
    for b in range(PER):
        here = by_block[b * coarse : (b + 1) * coarse]
        come, go = iota((drift, width), 0) * PER + b, position(iota((drift, width), 1))
        before = jnp.dot(here, hot(come < go), preferred_element_type=F32)
        same = jnp.dot(here, hot(come == go), preferred_element_type=F32)
        ranks = before if b == 0 else ranks + before
        set_here = same if b == 0 else set_here + same
    rank[...] = jnp.where(set_here > 0, ranks, -1.0)
    filled[...] = jnp.broadcast_to(jnp.sum(set_here, axis=1, keepdims=True), filled.shape)

    early = [m for m in (4, 3, 2, 1) if m <= REACH and m < far]
    middle = [m for m in (6, 5) if REACH < m <= 2 * REACH and m < far]
    late = [m for m in range(far - 1, 0, -1) if m not in early + middle]

    def ways(ms):
        return [d for m in ms for d in (m, n - m)]

    at = iota((8, width), 1)
    code = (position(at) + 1).astype(F32).astype(BF16)
    slot_wide = iota((CAP, width), 0).astype(F32)
    slot = iota((CAP, BLOCK), 0).astype(F32)
    lane = iota((1, BLOCK), 1)

    def choose(c):
        chosen = hot(slot_wide == rank[pl.ds(c, 1), :])
        blocks = spec[:, pl.ds(c * PER, PER)].reshape(width, BLOCK)
        return jnp.dot(chosen, blocks, preferred_element_type=F32), dot_nt(code, chosen)[0:1]

    def build(c):
        power, codes = choose(c)
        normal = (power - mean[pl.ds(c, 1), :]) / sigma[pl.ds(c, 1), :]
        return jnp.where(slot < filled[pl.ds(c, 1), :], normal, 0.0).astype(BF16), codes

    def pack(d):
        payload, codes = build(source_of[(me + d) % n])
        send_rows[d] = payload
        send_codes[d] = codes

    def copies(send_buffer, buffer, sems):
        def copy(d):
            return pltpu.make_async_remote_copy(
                src_ref=send_buffer.at[d], dst_ref=buffer.at[me],
                send_sem=sems.at[0, d], recv_sem=sems.at[1, d],
                device_id={"freq": (me + d) % n}, device_id_type=MESH,
            )
        return copy

    row_copy = copies(send_rows, rows, row_sems)
    code_copy = copies(send_codes, got_codes, code_sems)
    norm_copy = copies(send_norms, got_norms, norm_sems)

    def send(d):
        code_copy(d).start()
        row_copy(d).start()

    def each_late(act):
        act(far)
        at = 0
        while at < len(late):
            size = next((k for k in range(1, len(late) - at) if late[at + k] != late[at] - k), len(late) - at)
            if size > 2:
                def body(k, carry, top=late[at]):
                    act(top - k)
                    act(n - top + k)
                    return carry
                lax.fori_loop(0, size, body, 0)
            else:
                for d in ways(late[at : at + size]):
                    act(d)
            at += size

    def tell(k):
        if k < rounds:
            for to in (me + REACH, me + n - REACH):
                pl.semaphore_signal(chain.at[k], inc=1, device_id={"freq": to % n}, device_id_type=MESH)

    def hear(k):
        if k < rounds:
            pl.semaphore_wait(chain.at[k], 2)
            tell(k + 1)

    owned = [owner[k] for k in range(coarse)]
    sources = []
    for d in ways(early):
        wanted, found = (me + d) % n * coarse + me, 0
        for k in range(coarse):
            found = jnp.where(owned[k] == wanted, k, found)
        sources.append(found)
    for copy in large:
        copy.wait()
    for d, c in zip(ways(early), sources):
        power, codes = choose(c)
        send_rows[d] = power.astype(BF16)
        send_codes[d] = codes
    pl.semaphore_wait(barrier, 2 * REACH + 1)
    tell(0)
    for d in ways(early):
        send(d)

    def stats(c, carry):
        center = BIN_STEP * median[c].astype(F32)
        deviation = mad[c].astype(F32)
        wide = MAD_WIDTH * BIN_STEP * deviation
        mean[pl.ds(c, 1), :] = jnp.full((1, BLOCK), center, F32)
        sigma[pl.ds(c, 1), :] = jnp.full((1, BLOCK), MAD_SCALE * BIN_STEP * deviation, F32)
        found = 0
        for k in range(coarse):
            found = jnp.where(owner[k] == c * coarse + me, k, found)
        source_of[c] = found
        x = spec[:, pl.ds(c * PER, PER)].astype(F32)
        inside = (x >= center - wide) & (x <= center + wide)
        kept = jnp.where(inside, x - center, 0.0)
        for k, each in enumerate((jnp.where(inside, 1.0, 0.0), kept, kept * kept)):
            mine[k, pl.ds(c, 1), :] = jnp.sum(jnp.sum(each, axis=(0, 1)), axis=0, keepdims=True)
        return carry

    lax.fori_loop(0, coarse, stats, 0, unroll=2)
    hear(0)
    share = pltpu.make_async_remote_copy(
        src_ref=mine, dst_ref=theirs, send_sem=stat_sems.at[0], recv_sem=stat_sems.at[1],
        device_id={"sub": 1 - half}, device_id_type=MESH,
    )
    share.start()
    share.wait()
    total = [jnp.sum(mine[k] + theirs[k], axis=1, keepdims=True) for k in range(3)]
    floor = jnp.maximum(total[0], 1.0)
    mean[...] = mean[...] + total[1] / floor
    sigma[...] = jnp.sqrt(0.5 * total[2] / floor + 0.5 * sigma[...] * sigma[...])
    for d, c in zip(ways(early), sources):
        send_norms[d] = jnp.where(lane < BLOCK // 2, mean[pl.ds(c, 1), :], sigma[pl.ds(c, 1), :])
    for d in ways(middle):
        pack(d)
    for d in ways(early):
        norm_copy(d).start()
    for d in ways(middle):
        send(d)
    hear(1)
    each_late(pack)
    for k in range(2, rounds):
        hear(k)
    each_late(lambda d: code_copy(d).start())
    each_late(lambda d: row_copy(d).start())

    ones = jnp.ones((8, BLOCK), BF16)

    def sender(d):
        return (me + n - d) % n

    def take_codes(s):
        codes = got_codes[s]
        base = (s * total_drift + half * drift) * PER - 1
        keys[pl.ds(s, 1), :] = jnp.where(codes > 0, codes + base.astype(F32), -1.0)

    def take_rows(s):
        over = jnp.maximum(rows[s].astype(F32) - THRESH, 0.0)
        coarse_part = over.astype(BF16)
        left = over - coarse_part.astype(F32)
        fine_part = jnp.where(left == left, left, 0.0).astype(BF16)
        excess[pl.ds(s, 1), :] = (dot_nt(ones, coarse_part) + dot_nt(ones, fine_part))[0:1]

    def codes_in(d):
        code_copy(d).wait()
        take_codes(sender(d))

    def rows_in(d):
        row_copy(d).wait()
        take_rows(sender(d))

    payload, codes = build(source_of[me])
    rows[me] = payload
    got_codes[me] = codes
    take_codes(me)
    take_rows(me)
    for d in ways(early):
        s = sender(d)
        codes_in(d)
        row_copy(d).wait()
        norm_copy(d).wait()
        live = jnp.sum(jnp.where(got_codes[s] > 0, 1.0, 0.0), axis=1, keepdims=True)
        norms = got_norms[s]
        normal = (rows[s].astype(F32) - norms[:, 0:1]) / norms[:, BLOCK // 2 : BLOCK // 2 + 1]
        rows[s] = jnp.where(slot < live, normal, 0.0).astype(BF16)
        take_rows(s)
    for d in ways(middle):
        codes_in(d)
        rows_in(d)
    each_late(codes_in)
    counts = dot_nt(ones, hot(keys[...] >= 0))
    earlier = hot(iota((n, n), 0) < iota((n, n), 1))
    begins[...] = jnp.dot(counts.astype(BF16), earlier, preferred_element_type=F32).astype(jnp.int32)
    each_late(rows_in)


def compact_kernel(
    n, begins_vmem, rows, keys, excess, snr_out, keys_out, excess_out, wide, narrow, key_rows, excess_rows, key_ints, begins, sems
):
    fetch = pltpu.make_async_copy(begins_vmem, begins, sems.at[0])
    fetch.start()
    wide[...] = jnp.zeros_like(wide)
    key_rows[...] = jnp.full_like(key_rows, -1.0)
    excess_rows[...] = jnp.zeros_like(excess_rows)
    lane = lax.broadcasted_iota(jnp.int32, (1, BLOCK), 1)
    fetch.wait()
    for s in range(n):
        begin = begins[0, s]
        wide[pl.ds(begin, CAP), :] = rows[s].astype(F32)
        row, shift = lax.div(begin, BLOCK), lax.rem(begin, BLOCK)
        for source, target, empty in ((keys, key_rows, -1.0), (excess, excess_rows, 0.0)):
            turned = pltpu.roll(source[pl.ds(s, 1), :], shift, 1)
            here, after = pl.ds(row, 1), pl.ds(row + 1, 1)
            target[here, :] = jnp.where(lane >= shift, turned, target[here, :])
            target[after, :] = jnp.where(lane < shift, turned, empty)
    key_ints[...] = key_rows[0:n, :].astype(jnp.int32)
    parts = sems.shape[0] - 3
    size = n * CAP // parts
    writes = [
        pltpu.make_async_copy(key_ints, keys_out, sems.at[parts + 1]),
        pltpu.make_async_copy(excess_rows.at[pl.ds(0, n), :], excess_out, sems.at[parts + 2]),
    ]
    for k in range(parts):
        part = pl.ds(k * size, size)
        narrow[part, :] = wide[part, :].astype(BF16)
        writes.append(pltpu.make_async_copy(narrow.at[part, :], snr_out.at[part, :], sems.at[k + 1]))
        if k == 1:
            writes[0].start()
            writes[1].start()
        if k:
            writes[k + 1].start()
    writes[-1].start()
    for write in writes:
        write.wait()


def per_device(spectrum, hit_mask, owner_map, median_bin, mad_bin):
    drift = spectrum.shape[0]
    coarse = owner_map.shape[0]
    n = lax.axis_size("freq")
    total_drift = drift * lax.axis_size("sub")
    width = PER * drift
    vmem = pl.BlockSpec(memory_space=VMEM)
    tiles = spectrum.reshape(drift // 8, 8, coarse * PER, BLOCK).transpose(0, 2, 1, 3)
    table, line = VMEM((coarse, BLOCK), F32), VMEM((n, 1, CAP), F32)
    dma = pltpu.SemaphoreType.DMA
    rows, keys, excess, begins = pl.pallas_call(
        functools.partial(exchange_kernel, n, coarse, drift, total_drift),
        out_shape=[
            jax.ShapeDtypeStruct((n, CAP, BLOCK), BF16),
            jax.ShapeDtypeStruct((n, BLOCK), F32),
            jax.ShapeDtypeStruct((n, BLOCK), F32),
            jax.ShapeDtypeStruct((8, n), jnp.int32),
        ],
        in_specs=[pl.BlockSpec(memory_space=pltpu.HBM)] * 5,
        out_specs=[vmem] * 4,
        scratch_shapes=[
            SMEM((coarse,), jnp.int32), SMEM((coarse,), jnp.int32), SMEM((coarse,), jnp.int32),
            SMEM((coarse,), jnp.int32),
            VMEM(hit_mask.shape, jnp.int32), VMEM(tiles.shape, BF16),
            VMEM((3, coarse, BLOCK), F32), VMEM((3, coarse, BLOCK), F32), table, table,
            VMEM((coarse, width), F32), table,
            VMEM((n, CAP, BLOCK), BF16), line, line, line, line,
            dma((4,)), dma((4,)), dma((2,)), dma((2, n)), dma((2, n)), dma((2, n)),
            pltpu.SemaphoreType.REGULAR((max(n // 2 // REACH - 1, 1),)),
        ],
        compiler_params=pltpu.CompilerParams(
            collective_id=0, has_side_effects=True, vmem_limit_bytes=16 * 1024 * 1024
        ),
        name="exchange",
    )(*(pltpu.with_memory_space_constraint(x, pltpu.HBM) for x in (owner_map, median_bin, mad_bin, hit_mask, tiles)))
    snr, keys, excess = pl.pallas_call(
        functools.partial(compact_kernel, n),
        out_shape=[
            jax.ShapeDtypeStruct((n * CAP, BLOCK), BF16),
            jax.ShapeDtypeStruct((n, BLOCK), jnp.int32),
            jax.ShapeDtypeStruct((n, BLOCK), F32),
        ],
        in_specs=[vmem] * 4,
        out_specs=[pl.BlockSpec(memory_space=pltpu.HBM)] * 3,
        scratch_shapes=[
            VMEM((n * CAP, BLOCK), F32), VMEM((n * CAP, BLOCK), BF16),
            VMEM((n + 8, BLOCK), F32), VMEM((n + 8, BLOCK), F32), VMEM((n, BLOCK), jnp.int32),
            SMEM((8, n), jnp.int32), dma((7,)),
        ],
        compiler_params=pltpu.CompilerParams(vmem_limit_bytes=16 * 1024 * 1024),
        name="compact",
    )(begins, rows, keys, excess)
    total = n * CAP
    return snr.reshape(1, 1, total, BLOCK), keys.reshape(1, 1, total), excess.reshape(1, 1, total)


def solution(mesh):
    placed = (
        P("sub", ("beam", "freq")),
        P("sub", ("beam", "freq")),
        P(("beam", "freq")),
        P(("beam", "freq")),
        P(("beam", "freq")),
    )
    return jax.shard_map(
        per_device,
        mesh=mesh,
        in_specs=placed,
        out_specs=(
            P("freq", "sub", "beam", None),
            P("freq", "sub", "beam"),
            P("freq", "sub", "beam"),
        ),
        check_vma=False,
    )
```
